8 devices in a mesh: dp: 1 (over z), tp: 2 (over y), ep: 4 (over x, core).
Axes of the slice: x: 2, y: 2, z: 1, core: 2. Of those that a mesh axis runs over, the one named last changes fastest.
Arguments:
- tokens: bfloat16 [4096, 2048], P(('dp', 'ep', 'tp'))
- expert_ids: int32 [4096, 4], P(('dp', 'ep', 'tp'))
- gates: float32 [4096, 4], P(('dp', 'ep', 'tp'))
- slots: int32 [4096, 4], P(('dp', 'ep', 'tp'))
- shared_w1: bfloat16 [2048, 5632], P(None, 'tp')
- shared_w3: bfloat16 [2048, 5632], P(None, 'tp')
- shared_w2: bfloat16 [5632, 2048], P('tp')
- expert_w1: bfloat16 [60, 2048, 1408], P('ep')
- expert_w3: bfloat16 [60, 2048, 1408], P('ep')
- expert_w2: bfloat16 [60, 1408, 2048], P('ep')
Outputs:
- output: bfloat16 [4096, 2048], P(('dp', 'ep', 'tp'))
All inputs are finite; a program needn't handle non-finite values.
Results may differ from the reference program's by a relative error of at most 0.00136.
Values are sent between devices in bfloat16 or wider.
A program may use at most 1.25 GiB of HBM per device.

```python
import jax
import jax.numpy as jnp
from jax import lax

D_MODEL = 2048
FF_EXPERT = 1408
FF_SHARED = 5632
EXPERTS = 60
TOP_K = 4
TOKENS_DEV = 512
EP_SIZE = 4
TP_SIZE = 2
CAPACITY = 72

N_SOURCES = EP_SIZE * TP_SIZE
N_TOKENS = N_SOURCES * TOKENS_DEV


def draw_routing(route_key):
    key_hot, key_score = jax.random.split(route_key)
    hot_ids = jax.random.randint(key_hot, (2,), 0, EXPERTS)
    expert_range = jnp.arange(EXPERTS, dtype=jnp.int32)
    scores = jax.random.randint(key_score, (N_TOKENS, EXPERTS), 0, 1024)
    favoured = jnp.any(expert_range[None, :] == hot_ids[:, None], axis=0).astype(jnp.int32) * 128
    row_pos = jnp.arange(N_TOKENS, dtype=jnp.int32) % TOKENS_DEV
    forced = ((row_pos[:, None] < CAPACITY) & (expert_range[None, :] == hot_ids[0])).astype(jnp.int32) * 4096
    keyed_scores = (scores + favoured[None, :] + forced) * EXPERTS + expert_range[None, :]
    top_vals, expert_ids = lax.top_k(keyed_scores, TOP_K)
    expert_ids = expert_ids.astype(jnp.int32)
    per_source = expert_ids.reshape(N_SOURCES, TOKENS_DEV * TOP_K)
    one_hot = (per_source[:, :, None] == expert_range[None, None, :]).astype(jnp.int32)
    position = jnp.sum(jnp.cumsum(one_hot, axis=1) * one_hot, axis=2) - 1
    slots = jnp.where(position < CAPACITY, position, -1)
    return expert_ids, slots.reshape(N_TOKENS, TOP_K).astype(jnp.int32)


def normal_weights(weight_key, shape, fan_in):
    return (jax.random.normal(weight_key, shape, jnp.float32) * fan_in ** -0.5).astype(jnp.bfloat16)


def setup_inputs(seed: int = 0, part: int = 0) -> dict:
    root_key = jax.random.key(seed)
    shared_key, base_key = jax.random.split(root_key)
    part_key = jax.random.fold_in(base_key, part)
    key_tok, key_route, key_gate = jax.random.split(part_key, 3)
    key_list = jax.random.split(shared_key, 6)
    tokens = jax.random.normal(key_tok, (N_TOKENS, D_MODEL), jnp.float32).astype(jnp.bfloat16)
    expert_ids, slots = draw_routing(key_route)
    gates = jax.random.uniform(key_gate, (N_TOKENS, TOP_K), jnp.float32, 0.5, 1.0)
    return {
        "tokens": tokens,
        "expert_ids": expert_ids,
        "gates": gates,
        "slots": slots,
        "shared_w1": normal_weights(key_list[0], (D_MODEL, FF_SHARED), D_MODEL),
        "shared_w3": normal_weights(key_list[1], (D_MODEL, FF_SHARED), D_MODEL),
        "shared_w2": normal_weights(key_list[2], (FF_SHARED, D_MODEL), FF_SHARED),
        "expert_w1": normal_weights(key_list[3], (EXPERTS, D_MODEL, FF_EXPERT), D_MODEL),
        "expert_w3": normal_weights(key_list[4], (EXPERTS, D_MODEL, FF_EXPERT), D_MODEL),
        "expert_w2": normal_weights(key_list[5], (EXPERTS, FF_EXPERT, D_MODEL), FF_EXPERT),
    }


def swiglu_rows(token_rows, w_gate, w_up, w_down):
    gate_pre = jnp.dot(token_rows, w_gate, preferred_element_type=jnp.float32)
    up_pre = jnp.dot(token_rows, w_up, preferred_element_type=jnp.float32)
    hidden = (jax.nn.silu(gate_pre) * up_pre).astype(jnp.bfloat16)
    return jnp.dot(hidden, w_down, preferred_element_type=jnp.float32)


def reference(tokens, expert_ids, gates, slots, shared_w1, shared_w3, shared_w2, expert_w1, expert_w3, expert_w2):
    token_blocks = tokens.reshape(N_SOURCES, TOKENS_DEV, D_MODEL)

    def shared_block(block_rows):
        return swiglu_rows(block_rows, shared_w1, shared_w3, shared_w2)

    shared_out = lax.map(shared_block, token_blocks).reshape(N_TOKENS, D_MODEL)

    tok_ids = jnp.arange(N_TOKENS, dtype=jnp.int32)
    flat_tok = jnp.repeat(tok_ids, TOP_K)
    flat_src = flat_tok // TOKENS_DEV
    flat_exp = expert_ids.reshape(-1)
    flat_slot = jnp.where(slots.reshape(-1) >= 0, slots.reshape(-1), CAPACITY)
    inv_tok = jnp.full((EXPERTS, N_SOURCES, CAPACITY), N_TOKENS, jnp.int32).at[flat_exp, flat_src, flat_slot].set(flat_tok, mode="drop")
    inv_gate = jnp.zeros((EXPERTS, N_SOURCES, CAPACITY), jnp.float32).at[flat_exp, flat_src, flat_slot].set(gates.reshape(-1), mode="drop")

    def expert_step(accum_sum, step_inputs):
        rows_tok, rows_gate, w_gate, w_up, w_down = step_inputs
        tok_flat = rows_tok.reshape(-1)
        token_rows = jnp.take(tokens, tok_flat, axis=0, mode="fill", fill_value=0)
        expert_out = swiglu_rows(token_rows, w_gate, w_up, w_down).astype(jnp.bfloat16)
        weighted = rows_gate.reshape(-1)[:, None] * expert_out.astype(jnp.float32)
        return accum_sum.at[tok_flat].add(weighted, mode="drop"), None

    routed, unused_out = lax.scan(expert_step, jnp.zeros((N_TOKENS, D_MODEL), jnp.float32), (inv_tok, inv_gate, expert_w1, expert_w3, expert_w2))
    y_total = tokens.astype(jnp.float32) + shared_out + routed
    return y_total.astype(jnp.bfloat16)
```

```python
import functools

import jax
import jax.numpy as jnp
from jax import lax
from jax.experimental import pallas as pl
from jax.experimental.pallas import tpu as pltpu
from jax.sharding import PartitionSpec as P

COL_BLOCKS = 4
GATE_MAX = 3.3895313892515355e38


def capacity_rows(tok_dev, top_k, n_exp):
    return 8 * max(1, (2 * tok_dev * top_k + 8 * n_exp - 1) // (8 * n_exp))


def swiglu_rows(token_rows, w_gate, w_up, w_down):
    gate_pre = jnp.dot(token_rows, w_gate, preferred_element_type=jnp.float32)
    up_pre = jnp.dot(token_rows, w_up, preferred_element_type=jnp.float32)
    hidden = (jax.nn.silu(gate_pre) * up_pre).astype(jnp.bfloat16)
    return jnp.dot(hidden, w_down, preferred_element_type=jnp.float32)


def params(mib):
    return pltpu.CompilerParams(vmem_limit_bytes=mib * 2**20)


def gather_kernel(cap, group, code_ref, first_ref, second_ref, out_ref):
    rows = group * cap
    slot = lax.broadcasted_iota(jnp.int32, (rows, code_ref.shape[2]), 0) + pl.program_id(0) * rows
    for source, tok_ref in enumerate((first_ref, second_ref)):
        code = code_ref[source]
        hit = slot == code[0:1, :]
        for j in range(1, code.shape[0]):
            hit = hit | (slot == code[j : j + 1, :])
        pick = jnp.where(hit, 1.0, 0.0).astype(jnp.bfloat16)
        picked = jnp.dot(pick, tok_ref[...], preferred_element_type=jnp.float32).astype(jnp.bfloat16)
        for k in range(group):
            out_ref[k, source * cap : (source + 1) * cap, :] = picked[k * cap : (k + 1) * cap, :]


def gather_rows(codes, first, second, local_exp, cap):
    tok_dev, d_model = first.shape
    group = 3
    rows = 2 * local_exp * cap
    return pl.pallas_call(
        functools.partial(gather_kernel, cap, group),
        grid=(local_exp // group,),
        out_shape=jax.ShapeDtypeStruct((local_exp, 2 * cap, d_model), jnp.bfloat16),
        in_specs=[
            pl.BlockSpec(codes.shape, lambda b: (0, 0, 0)),
            pl.BlockSpec((tok_dev, d_model), lambda b: (0, 0)),
            pl.BlockSpec((tok_dev, d_model), lambda b: (0, 0)),
        ],
        out_specs=pl.BlockSpec((group, 2 * cap, d_model), lambda b: (b, 0, 0)),
        compiler_params=params(40),
        cost_estimate=pl.CostEstimate(flops=2 * rows * tok_dev * d_model, bytes_accessed=2 * rows * d_model, transcendentals=0),
        name="gather_rows",
    )(codes, first, second)


def combine_kernel(cap, code_ref, gate_ref, out_ref):
    rows, top_k = code_ref.shape
    width = 3 * cap
    lane = lax.broadcasted_iota(jnp.int32, (rows, width), 1)
    piece = (lane >= cap).astype(jnp.int32) + (lane >= 2 * cap).astype(jnp.int32)
    target = lane - piece * cap + pl.program_id(0) * cap
    value = jnp.zeros((rows, width), jnp.float32)
    for j in range(top_k):
        value = jnp.where(target == code_ref[:, j : j + 1], gate_ref[:, j : j + 1], value)
    high = jnp.minimum(value, GATE_MAX).astype(jnp.bfloat16).astype(jnp.float32)
    rest = value - high
    middle = rest.astype(jnp.bfloat16).astype(jnp.float32)
    low = rest - middle
    out_ref[0] = jnp.where(piece == 0, high, jnp.where(piece == 1, middle, low)).astype(jnp.bfloat16)


def combine_matrix(code_cols, gate_cols, local_exp, cap):
    rows, top_k = code_cols.shape
    return pl.pallas_call(
        functools.partial(combine_kernel, cap),
        grid=(local_exp,),
        out_shape=jax.ShapeDtypeStruct((local_exp, rows, 3 * cap), jnp.bfloat16),
        in_specs=[pl.BlockSpec((rows, top_k), lambda e: (0, 0))] * 2,
        out_specs=pl.BlockSpec((1, rows, 3 * cap), lambda e: (e, 0, 0)),
        compiler_params=params(40),
        cost_estimate=pl.CostEstimate(flops=local_exp * rows * 3 * cap * 400, bytes_accessed=local_exp * rows * 512, transcendentals=0),
        name="combine_matrix",
    )(code_cols, gate_cols)


def hidden_kernel(near_ref, far_ref, gate_w_ref, up_w_ref, out_ref):
    rows = jnp.concatenate([near_ref[0], far_ref[0]], axis=0)
    width = out_ref.shape[2]
    step = 256
    for start in range(0, width, step):
        cols = slice(start, min(start + step, width))
        gate_pre = jnp.dot(rows, gate_w_ref[0, :, cols], preferred_element_type=jnp.float32)
        up_pre = jnp.dot(rows, up_w_ref[0, :, cols], preferred_element_type=jnp.float32)
        out_ref[0, :, cols] = (jax.nn.silu(gate_pre) * up_pre).astype(jnp.bfloat16)


def expert_hidden(near, far, w_gate, w_up):
    local_exp, half, d_model = near.shape
    width = w_gate.shape[2]
    row_spec = pl.BlockSpec((1, half, d_model), lambda e: (e, 0, 0))
    weight_spec = pl.BlockSpec((1, d_model, width), lambda e: (e, 0, 0))
    return pl.pallas_call(
        hidden_kernel,
        grid=(local_exp,),
        out_shape=jax.ShapeDtypeStruct((local_exp, 2 * half, width), jnp.bfloat16),
        in_specs=[row_spec, row_spec, weight_spec, weight_spec],
        out_specs=pl.BlockSpec((1, 2 * half, width), lambda e: (e, 0, 0)),
        compiler_params=params(56),
        cost_estimate=pl.CostEstimate(
            flops=local_exp * 2 * half * d_model * width * 4,
            bytes_accessed=local_exp * d_model * width * 4,
            transcendentals=local_exp * 2 * half * width,
        ),
        name="expert_hidden",
    )(near, far, w_gate, w_up)


def partial_kernel(cap, tok_dev, hidden_ref, weight_ref, combine_ref, out_ref):
    result = jnp.dot(hidden_ref[0], weight_ref[0], preferred_element_type=jnp.float32)
    n_sources = out_ref.shape[0]

    @pl.when(pl.program_id(0) == 0)
    def _():
        out_ref[...] = jnp.zeros_like(out_ref)

    for source in range(n_sources):
        part = result[source * cap : (source + 1) * cap, :].astype(jnp.bfloat16).astype(jnp.float32)
        stacked = jnp.concatenate([part, part, part], axis=0).astype(jnp.bfloat16)
        weights = combine_ref[0, source * tok_dev : (source + 1) * tok_dev, :]
        out_ref[source] += jnp.dot(weights, stacked, preferred_element_type=jnp.float32)


def expert_partial(hidden, w_down, combine, n_sources, block, n_blocks):
    local_exp, rows, width = hidden.shape
    cap = rows // n_sources
    tok_dev = combine.shape[1] // n_sources
    cols = w_down.shape[2] // n_blocks
    return pl.pallas_call(
        functools.partial(partial_kernel, cap, tok_dev),
        grid=(local_exp,),
        out_shape=jax.ShapeDtypeStruct((n_sources, tok_dev, cols), jnp.float32),
        in_specs=[
            pl.BlockSpec((1, rows, width), lambda e: (e, 0, 0)),
            pl.BlockSpec((1, width, cols), lambda e: (e, 0, block)),
            pl.BlockSpec((1, n_sources * tok_dev, 3 * cap), lambda e: (e, 0, 0)),
        ],
        out_specs=pl.BlockSpec((n_sources, tok_dev, cols), lambda e: (0, 0, 0)),
        compiler_params=params(40),
        cost_estimate=pl.CostEstimate(
            flops=2 * local_exp * cols * (rows * width + n_sources * tok_dev * 256),
            bytes_accessed=local_exp * 2 * (width * cols + rows * width + n_sources * tok_dev * 256),
            transcendentals=0,
        ),
        name="expert_partial",
    )(hidden, w_down, combine)


def solution(mesh):
    ep_size = mesh.shape["ep"]
    tp_size = mesh.shape["tp"]
    row_spec = P(("dp", "ep", "tp"), None)
    expert_spec = P("ep", None, None)
    core_swap = [(i, i ^ 1) for i in range(ep_size)]
    chip_swap = [(i, i ^ 2) for i in range(ep_size)]
    both_swap = [(i, i ^ 3) for i in range(ep_size)]
    tp_swap = [(i, i ^ 1) for i in range(tp_size)]

    def local_layer(tokens, expert_ids, gates, slots, shared_w1, shared_w3, shared_w2, expert_w1, expert_w3, expert_w2):
        tok_dev, d_model = tokens.shape
        top_k = expert_ids.shape[1]
        local_exp = expert_w1.shape[0]
        cap = capacity_rows(tok_dev, top_k, local_exp * ep_size)
        me = lax.axis_index("ep")

        code = jnp.where(slots >= 0, expert_ids * cap + slots, -1)
        meta = jnp.concatenate([code.astype(jnp.float32).T, gates.T], axis=0)
        metas = [meta] + [lax.ppermute(meta, "ep", perm) for perm in (core_swap, chip_swap, both_swap)]
        metas = jnp.stack(metas)
        codes = metas[:, :top_k].astype(jnp.int32)
        mine = (codes >= 0) & (codes // (local_exp * cap) == me)
        codes = jnp.where(mine, codes - me * (local_exp * cap), -1)
        code_cols = codes.transpose(0, 2, 1).reshape(ep_size * tok_dev, top_k)
        gate_cols = metas[:, top_k:].transpose(0, 2, 1).reshape(ep_size * tok_dev, top_k)

        other_tp = lax.ppermute(tokens, "tp", tp_swap)
        tok_core = lax.ppermute(tokens, "ep", core_swap)
        tok_chip = lax.ppermute(tokens, "ep", chip_swap)
        tok_both = lax.ppermute(tok_chip, "ep", core_swap)

        shared_own = swiglu_rows(tokens, shared_w1, shared_w3, shared_w2)
        shared_other = swiglu_rows(other_tp, shared_w1, shared_w3, shared_w2)
        shared_back = lax.ppermute(shared_other, "tp", tp_swap)

        combine = combine_matrix(code_cols, gate_cols, local_exp, cap)
        near = gather_rows(codes[:2], tokens, tok_core, local_exp, cap)
        far = gather_rows(codes[2:], tok_chip, tok_both, local_exp, cap)
        hidden = expert_hidden(near, far, expert_w1, expert_w3)

        n_blocks = COL_BLOCKS
        cols = d_model // n_blocks
        outs = []
        for block in range(n_blocks):
            part = expert_partial(hidden, expert_w2, combine, ep_size, block, n_blocks)
            from_core = lax.ppermute(part[1::2], "ep", core_swap)
            for_chip = part[2] + from_core[1]
            from_chip = lax.ppermute(for_chip, "ep", chip_swap)
            here = slice(block * cols, (block + 1) * cols)
            routed = part[0] + from_core[0] + from_chip
            shared = shared_own[:, here] + shared_back[:, here]
            outs.append((tokens[:, here].astype(jnp.float32) + shared + routed).astype(jnp.bfloat16))
        return jnp.concatenate(outs, axis=1)

    return jax.shard_map(local_layer, mesh=mesh, in_specs=(row_spec, row_spec, row_spec, row_spec, P(None, "tp"), P(None, "tp"), P("tp", None), expert_spec, expert_spec, expert_spec), out_specs=row_spec, check_vma=False)
```

```python
import functools

import jax
import jax.numpy as jnp
from jax import lax
from jax.experimental import pallas as pl
from jax.experimental.pallas import tpu as pltpu
from jax.sharding import PartitionSpec as P

COL_BLOCKS = 8
GROUP = 3
FEW_SLOTS = 48
MESH = pl.DeviceIdType.MESH
GATE_MAX = 3.3895313892515355e38


def capacity_rows(tok_dev, top_k, n_exp):
    return 8 * max(1, (2 * tok_dev * top_k + 8 * n_exp - 1) // (8 * n_exp))


ANY = pl.BlockSpec(memory_space=pl.ANY)


def params():
    return pltpu.CompilerParams(vmem_limit_bytes=62 * 2**20)


def cost(flops, nbytes):
    return pl.CostEstimate(flops=flops, bytes_accessed=nbytes, transcendentals=0)


def gather_kernel(cap, few_ref, code_ref, first_ref, second_ref, after_ref, out_ref):
    rows = GROUP * cap
    base = pl.program_id(0) * GROUP
    slot = lax.broadcasted_iota(jnp.int32, (rows, code_ref.shape[2]), 0) + base * cap
    for source, tok_ref in enumerate((first_ref, second_ref)):
        code = code_ref[source]
        hit = slot == code[0:1, :]
        for j in range(1, code.shape[0]):
            hit = hit | (slot == code[j : j + 1, :])
        pick = jnp.where(hit, 1.0, 0.0).astype(jnp.bfloat16)
        picked = jnp.dot(pick, tok_ref[...], preferred_element_type=jnp.float32).astype(jnp.bfloat16)
        for k in range(GROUP):

            @pl.when(few_ref[base + k] == 1)
            def _():
                out_ref[k, source * FEW_SLOTS : (source + 1) * FEW_SLOTS, :] = picked[k * cap : k * cap + FEW_SLOTS, :]

            @pl.when(few_ref[base + k] == 0)
            def _():
                out_ref[k, source * cap : (source + 1) * cap, :] = picked[k * cap : (k + 1) * cap, :]


def gather_rows(few, codes, first, second, after, local_exp, cap):
    tok_dev, d_model = first.shape
    rows = 2 * local_exp * cap
    tok_spec = pl.BlockSpec((tok_dev, d_model), lambda b, few: (0, 0))
    return pl.pallas_call(
        functools.partial(gather_kernel, cap),
        grid_spec=pltpu.PrefetchScalarGridSpec(
            num_scalar_prefetch=1,
            grid=(local_exp // GROUP,),
            in_specs=[pl.BlockSpec(codes.shape, lambda b, few: (0, 0, 0)), tok_spec, tok_spec, ANY],
            out_specs=pl.BlockSpec((GROUP, 2 * cap, d_model), lambda b, few: (b, 0, 0)),
        ),
        out_shape=jax.ShapeDtypeStruct((local_exp, 2 * cap, d_model), jnp.bfloat16),
        compiler_params=params(),
        cost_estimate=cost(2 * rows * tok_dev * d_model, 2 * rows * d_model),
        name="gather_rows",
    )(few, codes, first, second, after)


def combine_kernel(cap, slot_ref, gate_ref, out_ref):
    gate = gate_ref[...]
    high = jnp.minimum(gate, GATE_MAX).astype(jnp.bfloat16).astype(jnp.float32)
    rest = gate - high
    middle = rest.astype(jnp.bfloat16).astype(jnp.float32)
    pieces = (high, middle, rest - middle)
    lane = lax.broadcasted_iota(jnp.int32, (gate.shape[0], 256), 1)
    for g in range(out_ref.shape[0]):
        values = [jnp.zeros(lane.shape, jnp.float32)] * 3
        for k in range(GROUP):
            e = g * GROUP + k
            hit = lane == slot_ref[:, e : e + 1] + k * cap
            values = [jnp.where(hit, piece[:, e : e + 1], value) for piece, value in zip(pieces, values)]
        for i, value in enumerate(values):
            out_ref[g, :, i * 256 : (i + 1) * 256] = value.astype(jnp.bfloat16)


def combine_matrix(slot_of, gate_of, cap):
    rows, local_exp = slot_of.shape
    step = 128
    n_groups = local_exp // GROUP
    in_spec = pl.BlockSpec((step, local_exp), lambda i: (i, 0))
    return pl.pallas_call(
        functools.partial(combine_kernel, cap),
        grid=(rows // step,),
        out_shape=jax.ShapeDtypeStruct((n_groups, rows, 768), jnp.bfloat16),
        in_specs=[in_spec, in_spec],
        out_specs=pl.BlockSpec((n_groups, step, 768), lambda i: (0, i, 0)),
        compiler_params=params(),
        cost_estimate=cost(n_groups * rows * 768 * 500, n_groups * rows * 1536),
        name="combine_matrix",
    )(slot_of, gate_of)


def swiglu_cols(rows, gate_w_ref, up_w_ref, cols):
    gate_pre = jnp.dot(rows, gate_w_ref[0, :, cols], preferred_element_type=jnp.float32)
    up_pre = jnp.dot(rows, up_w_ref[0, :, cols], preferred_element_type=jnp.float32)
    return jax.nn.silu(gate_pre) * up_pre


def hidden_kernel(cap, few_ref, near_ref, far_ref, gate_w_ref, up_w_ref, out_ref):
    few = few_ref[pl.program_id(0)]
    width = out_ref.shape[2]
    spans = [slice(start, min(start + 256, width)) for start in range(0, width, 256)]

    @pl.when(few == 1)
    def _():
        half = 2 * FEW_SLOTS
        rows = jnp.concatenate([near_ref[0, :half], far_ref[0, :half]], axis=0)
        for cols in spans:
            hidden = swiglu_cols(rows, gate_w_ref, up_w_ref, cols)
            gap = jnp.zeros((cap - FEW_SLOTS, hidden.shape[1]), jnp.float32)
            pieces = []
            for source in range(4):
                pieces += [hidden[source * FEW_SLOTS : (source + 1) * FEW_SLOTS], gap]
            out_ref[0, :, cols] = jnp.concatenate(pieces, axis=0).astype(jnp.bfloat16)

    @pl.when(few == 0)
    def _():
        rows = jnp.concatenate([near_ref[0], far_ref[0]], axis=0)
        for cols in spans:
            out_ref[0, :, cols] = swiglu_cols(rows, gate_w_ref, up_w_ref, cols).astype(jnp.bfloat16)


def expert_hidden(few, near, far, w_gate, w_up):
    local_exp, half, d_model = near.shape
    width = w_gate.shape[2]
    row_spec = pl.BlockSpec((1, half, d_model), lambda e, few: (e, 0, 0))
    weight_spec = pl.BlockSpec((1, d_model, width), lambda e, few: (e, 0, 0))
    return pl.pallas_call(
        functools.partial(hidden_kernel, half // 2),
        grid_spec=pltpu.PrefetchScalarGridSpec(
            num_scalar_prefetch=1,
            grid=(local_exp,),
            in_specs=[row_spec, row_spec, weight_spec, weight_spec],
            out_specs=pl.BlockSpec((1, 2 * half, width), lambda e, few: (e, 0, 0)),
        ),
        out_shape=jax.ShapeDtypeStruct((local_exp, 2 * half, width), jnp.bfloat16),
        compiler_params=params(),
        cost_estimate=cost(local_exp * 2 * half * d_model * width * 4, local_exp * d_model * width * 4),
        name="expert_hidden",
    )(few, near, far, w_gate, w_up)


def shared_hidden_kernel(row_ref, gate_w_ref, up_w_ref, after_ref, out_ref):
    rows = row_ref[...]
    gate_pre = jnp.dot(rows, gate_w_ref[...], preferred_element_type=jnp.float32)
    up_pre = jnp.dot(rows, up_w_ref[...], preferred_element_type=jnp.float32)
    out_ref[...] = (jax.nn.silu(gate_pre) * up_pre).astype(jnp.bfloat16)


def shared_hidden(rows, w_gate, w_up, after):
    n_rows, d_model = rows.shape
    width = w_gate.shape[1]
    step = 256
    weight_spec = pl.BlockSpec((d_model, step), lambda i: (0, i))
    return pl.pallas_call(
        shared_hidden_kernel,
        grid=(width // step,),
        out_shape=jax.ShapeDtypeStruct((n_rows, width), jnp.bfloat16),
        in_specs=[pl.BlockSpec((n_rows, d_model), lambda i: (0, 0)), weight_spec, weight_spec, ANY],
        out_specs=pl.BlockSpec((n_rows, step), lambda i: (0, i)),
        compiler_params=params(),
        cost_estimate=cost(4 * n_rows * d_model * width, 4 * d_model * width),
        name="shared_hidden",
    )(rows, w_gate, w_up, after)


def shared_down_kernel(hidden_ref, weight_ref, after_ref, out_ref):
    out_ref[...] = jnp.dot(hidden_ref[...], weight_ref[...], preferred_element_type=jnp.float32)


def shared_down(hidden, w_down, after):
    n_rows, width = hidden.shape
    d_model = w_down.shape[1]
    step = 512
    return pl.pallas_call(
        shared_down_kernel,
        grid=(d_model // step,),
        out_shape=jax.ShapeDtypeStruct((n_rows, d_model), jnp.float32),
        in_specs=[pl.BlockSpec((n_rows, width), lambda i: (0, 0)), pl.BlockSpec((width, step), lambda i: (0, i)), ANY],
        out_specs=pl.BlockSpec((n_rows, step), lambda i: (0, i)),
        compiler_params=params(),
        cost_estimate=cost(2 * n_rows * d_model * width, 2 * d_model * width + 4 * n_rows * d_model),
        name="shared_down",
    )(hidden, w_down, after)


def finish_kernel(
    cap, n_blocks, hidden_hbm, combine_hbm, base_ref, weight_ref, out_ref,
    hidden, combine, total, from_core, from_chip,
    hidden_sem, combine_sem, core_send, core_recv, chip_send, chip_recv,
):
    block, group = pl.program_id(0), pl.program_id(1)
    n_groups = pl.num_programs(1)
    last_group = n_groups - 1
    tok_dev, cols = base_ref.shape
    me = lax.axis_index("ep")
    dp, tp = lax.axis_index("dp"), lax.axis_index("tp")
    core = (dp, tp, me + 1 - 2 * lax.rem(me, 2))
    chip = (dp, tp, lax.rem(me + 2, 4))

    def load(g):
        return (
            pltpu.make_async_copy(hidden_hbm.at[pl.ds(g * GROUP, GROUP)], hidden.at[pl.ds(g * GROUP, GROUP)], hidden_sem.at[g]),
            pltpu.make_async_copy(combine_hbm.at[g], combine.at[g], combine_sem.at[g]),
        )

    def core_copy(n):
        return pltpu.make_async_remote_copy(
            src_ref=total.at[lax.rem(n, 2), pl.ds(2, 2)], dst_ref=from_core.at[n],
            send_sem=core_send.at[n], recv_sem=core_recv.at[n], device_id=core, device_id_type=MESH,
        )

    def chip_copy(n):
        return pltpu.make_async_remote_copy(
            src_ref=from_core.at[n, 1], dst_ref=from_chip.at[n],
            send_sem=chip_send.at[n], recv_sem=chip_recv.at[n], device_id=chip, device_id_type=MESH,
        )

    def forward(n):
        core_copy(n).wait()
        from_core[n] += total[lax.rem(n, 2), 0:2]
        chip_copy(n).start()

    def finalize(n):
        chip_copy(n).wait()
        here = pl.ds(pl.multiple_of(n * cols, cols), cols)
        out_ref[:, here] = (from_core[n, 0] + from_chip[n]).astype(jnp.bfloat16)

    @pl.when((block == 0) & (group == 0))
    def _():
        for g in range(hidden_sem.shape[0]):
            for copy in load(g):
                copy.start()
        barrier = pltpu.get_barrier_semaphore()
        for peer in (core, chip):
            pl.semaphore_signal(barrier, inc=1, device_id=peer, device_id_type=MESH)
        pl.semaphore_wait(barrier, 2)

    @pl.when(block == 0)
    def _():
        for copy in load(group):
            copy.wait()

    slot = lax.rem(block, 2)

    @pl.when(group == 0)
    def _():
        total[slot, 0] = base_ref[...]
        for s in range(1, 4):
            total[slot, s] = jnp.zeros((tok_dev, cols), jnp.float32)

    results = []
    for k in range(GROUP):
        results.append(jnp.dot(hidden[group * GROUP + k], weight_ref[k], preferred_element_type=jnp.float32))
    gap = jnp.zeros((256 - GROUP * cap, cols), jnp.float32)
    for source, place in enumerate((0, 2, 1, 3)):
        rows = jnp.concatenate([r[source * cap : (source + 1) * cap] for r in results] + [gap], axis=0).astype(jnp.bfloat16)
        rows = jnp.concatenate([rows, rows, rows], axis=0)
        gates = combine[group, source * tok_dev : (source + 1) * tok_dev, :]
        total[slot, place] += jnp.dot(gates, rows, preferred_element_type=jnp.float32)

    @pl.when((group == 1) & (block >= 1))
    def _():
        forward(block - 1)

    @pl.when((group == 3) & (block >= 4))
    def _():
        finalize(block - 4)

    @pl.when(group == last_group)
    def _():
        core_copy(block).start()

    @pl.when((group == last_group) & (block == n_blocks - 1))
    def _():
        forward(block)
        for n in range(n_blocks - 4, n_blocks):
            finalize(n)


def finish(hidden, combine, base, w_down):
    local_exp, rows, width = hidden.shape
    n_groups, _, depth = combine.shape
    tok_dev, d_model = base.shape
    cols = d_model // COL_BLOCKS
    sems = pltpu.SemaphoreType.DMA((COL_BLOCKS,))
    return pl.pallas_call(
        functools.partial(finish_kernel, rows // 4, COL_BLOCKS),
        grid=(COL_BLOCKS, n_groups),
        out_shape=jax.ShapeDtypeStruct((tok_dev, d_model), jnp.bfloat16),
        in_specs=[
            ANY,
            ANY,
            pl.BlockSpec((tok_dev, cols), lambda n, g: (0, n)),
            pl.BlockSpec((GROUP, width, cols), lambda n, g: (g, 0, n)),
        ],
        out_specs=pl.BlockSpec((tok_dev, d_model), lambda n, g: (0, 0)),
        scratch_shapes=[
            pltpu.VMEM(hidden.shape, jnp.bfloat16),
            pltpu.VMEM(combine.shape, jnp.bfloat16),
            pltpu.VMEM((2, 4, tok_dev, cols), jnp.float32),
            pltpu.VMEM((COL_BLOCKS, 2, tok_dev, cols), jnp.float32),
            pltpu.VMEM((COL_BLOCKS, tok_dev, cols), jnp.float32),
            pltpu.SemaphoreType.DMA((n_groups,)),
            pltpu.SemaphoreType.DMA((n_groups,)),
            sems, sems, sems, sems,
        ],
        compiler_params=pltpu.CompilerParams(
            collective_id=0, has_side_effects=True, vmem_limit_bytes=62 * 2**20, dimension_semantics=("arbitrary", "arbitrary")
        ),
        cost_estimate=cost(2 * d_model * local_exp * (rows * width + 4 * tok_dev * 256), 2 * local_exp * width * d_model),
        name="finish",
    )(hidden, combine, base, w_down)


def solution(mesh):
    ep_size = mesh.shape["ep"]
    tp_size = mesh.shape["tp"]
    row_spec = P(("dp", "ep", "tp"), None)
    expert_spec = P("ep", None, None)
    core_swap = [(i, i ^ 1) for i in range(ep_size)]
    chip_swap = [(i, i ^ 2) for i in range(ep_size)]
    both_swap = [(i, i ^ 3) for i in range(ep_size)]
    tp_swap = [(i, i ^ 1) for i in range(tp_size)]

    def local_layer(tokens, expert_ids, gates, slots, shared_w1, shared_w3, shared_w2, expert_w1, expert_w3, expert_w2):
        tok_dev, d_model = tokens.shape
        top_k = expert_ids.shape[1]
        local_exp = expert_w1.shape[0]
        cap = capacity_rows(tok_dev, top_k, local_exp * ep_size)
        me = lax.axis_index("ep")

        tok_core = lax.ppermute(tokens, "ep", core_swap)
        half = tok_dev // 2
        other_parts = [lax.ppermute(tokens[i * half : (i + 1) * half], "tp", tp_swap) for i in range(2)]
        tok_chip = lax.ppermute(tokens, "ep", chip_swap)
        tok_both = lax.ppermute(tok_chip, "ep", core_swap)

        code = jnp.where(slots >= 0, expert_ids * cap + slots, -1)
        meta = jnp.concatenate([code.astype(jnp.float32).T, gates.T], axis=0)
        metas = [meta] + [lax.ppermute(meta, "ep", perm) for perm in (core_swap, chip_swap, both_swap)]
        metas = jnp.stack(metas)
        codes = metas[:, :top_k].astype(jnp.int32)
        first = me * (local_exp * cap)
        codes = jnp.where((codes >= first) & (codes < first + local_exp * cap), codes - first, -1)
        experts = jnp.arange(local_exp, dtype=jnp.int32)[:, None, None, None] * cap
        inside = (codes[None] >= experts) & (codes[None] < experts + cap)
        slot_of = jnp.max(jnp.where(inside, codes[None] - experts, -1024), axis=2)
        gate_of = jnp.sum(jnp.where(inside, metas[None, :, top_k:], 0.0), axis=2)
        few = (jnp.max(slot_of, axis=(1, 2)) < FEW_SLOTS).astype(jnp.int32)
        slot_of = slot_of.reshape(local_exp, ep_size * tok_dev).T
        gate_of = gate_of.reshape(local_exp, ep_size * tok_dev).T

        combine = combine_matrix(slot_of, gate_of, cap)
        near = gather_rows(few, codes[:2], tokens, tok_core, combine, local_exp, cap)
        hidden_0 = shared_hidden(other_parts[0], shared_w1, shared_w3, near)
        back_0 = lax.ppermute(shared_down(hidden_0, shared_w2, hidden_0), "tp", tp_swap)
        hidden_own = shared_hidden(tokens, shared_w1, shared_w3, hidden_0)
        hidden_1 = shared_hidden(other_parts[1], shared_w1, shared_w3, hidden_own)
        down_1 = shared_down(hidden_1, shared_w2, tok_chip)
        back_1 = lax.ppermute(down_1, "tp", tp_swap)
        far = gather_rows(few, codes[2:], tok_chip, tok_both, down_1, local_exp, cap)
        hidden = expert_hidden(few, near, far, expert_w1, expert_w3)
        shared_own = shared_down(hidden_own, shared_w2, hidden)
        base = tokens.astype(jnp.float32) + shared_own + jnp.concatenate([back_0, back_1], axis=0)
        return finish(hidden, combine, base, expert_w2)

    return jax.shard_map(local_layer, mesh=mesh, in_specs=(row_spec, row_spec, row_spec, row_spec, P(None, "tp"), P(None, "tp"), P("tp", None), expert_spec, expert_spec, expert_spec), out_specs=row_spec, check_vma=False)
```

```python
import functools

import jax
import jax.numpy as jnp
from jax import lax
from jax.experimental import pallas as pl
from jax.experimental.pallas import tpu as pltpu
from jax.sharding import PartitionSpec as P

COL_BLOCKS = 8
GROUP = 3
FEW_SLOTS = 48
SPAN = 512
CHUNK = 128
MESH = pl.DeviceIdType.MESH
GATE_MAX = 3.3895313892515355e38


def capacity_rows(tok_dev, top_k, n_exp):
    return 8 * max(1, (2 * tok_dev * top_k + 8 * n_exp - 1) // (8 * n_exp))


ANY = pl.BlockSpec(memory_space=pl.ANY)


def params():
    return pltpu.CompilerParams(vmem_limit_bytes=62 * 2**20)


def cost(flops, nbytes):
    return pl.CostEstimate(flops=flops, bytes_accessed=nbytes, transcendentals=0)


def peers():
    dp, tp, me = lax.axis_index("dp"), lax.axis_index("tp"), lax.axis_index("ep")
    core = me + 1 - 2 * lax.rem(me, 2)
    chip = lax.rem(me + 2, 4)
    both = lax.rem(core + 2, 4)
    return (dp, tp, core), (dp, tp, chip), (dp, tp, both), (dp, 1 - tp, me)


def greet(devices):
    barrier = pltpu.get_barrier_semaphore()
    for device in devices:
        pl.semaphore_signal(barrier, inc=1, device_id=device, device_id_type=MESH)
    pl.semaphore_wait(barrier, len(devices))


def combine_chunk(cap, local_exp, meta, out_ref):
    top_k = meta.shape[0] // 2
    cols = meta.T
    base = (lax.broadcasted_iota(jnp.int32, (CHUNK, local_exp), 1) + lax.axis_index("ep") * local_exp) * cap
    base = base.astype(jnp.float32)
    slot_of = jnp.full(base.shape, -1024.0, jnp.float32)
    gate = jnp.zeros(base.shape, jnp.float32)
    for j in range(top_k):
        offset = cols[:, j : j + 1] - base
        inside = (offset >= 0.0) & (offset < float(cap))
        slot_of = jnp.where(inside, offset, slot_of)
        gate = jnp.where(inside, cols[:, top_k + j : top_k + j + 1], gate)
    slot_of = slot_of.astype(jnp.int32)
    high = jnp.minimum(gate, GATE_MAX).astype(jnp.bfloat16).astype(jnp.float32)
    rest = gate - high
    middle = rest.astype(jnp.bfloat16).astype(jnp.float32)
    pieces = (high, middle, rest - middle)
    lane = lax.broadcasted_iota(jnp.int32, (CHUNK, 256), 1)
    depth = out_ref.shape[1] // 3
    for g in range(depth // 256):
        values = [jnp.zeros(lane.shape, jnp.float32)] * 3
        for k in range(GROUP):
            e = g * GROUP + k
            hit = lane == slot_of[:, e : e + 1] + k * cap
            values = [jnp.where(hit, piece[:, e : e + 1], value) for piece, value in zip(pieces, values)]
        for i, value in enumerate(values):
            out_ref[:, i * depth + g * 256 : i * depth + (g + 1) * 256] = value.astype(jnp.bfloat16)


def start_kernel(
    cap, local_exp, meta_ref, tok_hbm, w_gate_hbm, w_up_hbm, w_down_hbm,
    metas, tok_core, tok_chip, tok_both, combine_hbm, base_hbm, peer_hidden,
    own, other, own_hidden, load_sem, send_sem, recv_sem,
):
    core, chip, both, tp = peers()
    tok_dev, d_model = own.shape
    width = peer_hidden.shape[1]

    def remote(src, dst, device, i):
        return pltpu.make_async_remote_copy(
            src_ref=src, dst_ref=dst, send_sem=send_sem.at[i], recv_sem=recv_sem.at[i], device_id=device, device_id_type=MESH
        )

    load = pltpu.make_async_copy(tok_hbm, own, load_sem)
    load.start()
    greet((core, chip, both, tp))
    meta_copies = [remote(meta_ref, metas.at[i + 1], device, i) for i, device in enumerate((core, chip, both))]
    for copy in meta_copies:
        copy.start()
    to_chip = remote(tok_hbm, tok_chip, chip, 3)
    to_tp = remote(tok_hbm, other, tp, 4)
    to_core = remote(tok_hbm, tok_core, core, 5)
    onward = remote(tok_chip, tok_both, core, 6)
    for copy in (to_chip, to_tp, to_core):
        copy.start()
    metas[0] = meta_ref[...]
    for copy in meta_copies:
        copy.wait()

    per_source = tok_dev // CHUNK

    def write_combine(index, out_ref):
        i = index.index[0]
        here = pl.ds(pl.multiple_of(lax.rem(i, per_source) * CHUNK, CHUNK), CHUNK)
        combine_chunk(cap, local_exp, metas[i // per_source, :, here], out_ref)

    pltpu.emit_pipeline(
        write_combine,
        grid=(4 * per_source,),
        out_specs=[pl.BlockSpec((CHUNK, combine_hbm.shape[1]), lambda i: (i, 0))],
        _explicit_indices=True,
    )(combine_hbm)

    def hidden_of(rows, result):
        def body(index, gate_w_ref, up_w_ref):
            gate_pre = jnp.dot(rows[...], gate_w_ref[...], preferred_element_type=jnp.float32)
            up_pre = jnp.dot(rows[...], up_w_ref[...], preferred_element_type=jnp.float32)
            here = pl.ds(pl.multiple_of(index.index[0] * 256, 256), 256)
            result[:, here] = (jax.nn.silu(gate_pre) * up_pre).astype(jnp.bfloat16)

        spec = pl.BlockSpec((d_model, 256), lambda i: (0, i))
        pltpu.emit_pipeline(body, grid=(width // 256,), in_specs=[spec, spec], _explicit_indices=True)(w_gate_hbm, w_up_hbm)

    load.wait()
    hidden_of(own, own_hidden)

    def down(index, weight_ref, out_ref):
        here = pl.ds(pl.multiple_of(index.index[0] * 512, 512), 512)
        result = jnp.dot(own_hidden[...], weight_ref[...], preferred_element_type=jnp.float32)
        out_ref[...] = own[:, here].astype(jnp.float32) + result

    pltpu.emit_pipeline(
        down,
        grid=(d_model // 512,),
        in_specs=[pl.BlockSpec((width, 512), lambda i: (0, i))],
        out_specs=[pl.BlockSpec((tok_dev, 512), lambda i: (0, i))],
        _explicit_indices=True,
    )(w_down_hbm, base_hbm)

    to_chip.wait()
    onward.start()
    to_tp.wait()
    hidden_of(other, peer_hidden)
    to_core.wait()
    onward.wait()


def start(meta, tokens, w_gate, w_up, w_down, cap, local_exp):
    tok_dev, d_model = tokens.shape
    width = w_gate.shape[1]
    vmem = pl.BlockSpec(memory_space=pltpu.VMEM)
    tok_shape = jax.ShapeDtypeStruct((tok_dev, d_model), jnp.bfloat16)
    return pl.pallas_call(
        functools.partial(start_kernel, cap, local_exp),
        out_shape=[
            jax.ShapeDtypeStruct((4,) + meta.shape, jnp.float32),
            tok_shape, tok_shape, tok_shape,
            jax.ShapeDtypeStruct((4 * tok_dev, local_exp // GROUP * 768), jnp.bfloat16),
            jax.ShapeDtypeStruct((tok_dev, d_model), jnp.float32),
            jax.ShapeDtypeStruct((tok_dev, width), jnp.bfloat16),
        ],
        in_specs=[vmem, ANY, ANY, ANY, ANY],
        out_specs=[vmem, ANY, ANY, ANY, ANY, ANY, vmem],
        scratch_shapes=[
            pltpu.VMEM((tok_dev, d_model), jnp.bfloat16),
            pltpu.VMEM((tok_dev, d_model), jnp.bfloat16),
            pltpu.VMEM((tok_dev, width), jnp.bfloat16),
            pltpu.SemaphoreType.DMA,
            pltpu.SemaphoreType.DMA((7,)),
            pltpu.SemaphoreType.DMA((7,)),
        ],
        compiler_params=pltpu.CompilerParams(collective_id=1, has_side_effects=True, vmem_limit_bytes=67043328),
        cost_estimate=cost(10 * tok_dev * d_model * width, 10 * d_model * width),
        name="start",
    )(meta, tokens, w_gate, w_up, w_down)


def swiglu_cols(rows, gate_w_ref, up_w_ref, cols):
    gate_pre = jnp.dot(rows, gate_w_ref[0, :, cols], preferred_element_type=jnp.float32)
    up_pre = jnp.dot(rows, up_w_ref[0, :, cols], preferred_element_type=jnp.float32)
    return jax.nn.silu(gate_pre) * up_pre


def hidden_kernel(cap, meta_ref, *refs):
    tok_refs, (gate_w_ref, up_w_ref, out_ref, row_ref) = refs[:4], refs[4:]
    e = pl.program_id(0)
    top_k = meta_ref.shape[1] // 2
    first = (lax.axis_index("ep") * pl.num_programs(0) + e) * cap
    slots = [meta_ref[source, :top_k].astype(jnp.int32) - first for source in range(4)]
    last = jnp.max(jnp.stack([jnp.where(slot < cap, slot, -1) for slot in slots]))
    width = out_ref.shape[2]
    spans = [slice(start, min(start + SPAN, width)) for start in range(0, width, SPAN)]

    def pick_rows(n_slots):
        picked = []
        for source, tok_ref in enumerate(tok_refs):
            slot = slots[source]
            row = lax.broadcasted_iota(jnp.int32, (n_slots, slot.shape[1]), 0)
            hit = row == slot[0:1, :]
            for j in range(1, top_k):
                hit = hit | (row == slot[j : j + 1, :])
            pick = jnp.where(hit, 1.0, 0.0).astype(jnp.bfloat16)
            picked.append(jnp.dot(pick, tok_ref[...], preferred_element_type=jnp.float32))
        row_ref[: 4 * n_slots] = jnp.concatenate(picked, axis=0).astype(jnp.bfloat16)

    @pl.when(last < FEW_SLOTS)
    def _():
        pick_rows(FEW_SLOTS)
        for cols in spans:
            hidden = swiglu_cols(row_ref[: 4 * FEW_SLOTS], gate_w_ref, up_w_ref, cols)
            gap = jnp.zeros((cap - FEW_SLOTS, hidden.shape[1]), jnp.float32)
            pieces = []
            for source in range(4):
                pieces += [hidden[source * FEW_SLOTS : (source + 1) * FEW_SLOTS], gap]
            out_ref[0, :, cols] = jnp.concatenate(pieces, axis=0).astype(jnp.bfloat16)

    @pl.when(last >= FEW_SLOTS)
    def _():
        pick_rows(cap)
        for cols in spans:
            out_ref[0, :, cols] = swiglu_cols(row_ref[...], gate_w_ref, up_w_ref, cols).astype(jnp.bfloat16)


def expert_hidden(metas, sources, w_gate, w_up, cap):
    local_exp, d_model, width = w_gate.shape
    tok_dev = sources[0].shape[0]
    rows = 4 * cap
    tok_spec = pl.BlockSpec((tok_dev, d_model), lambda e: (0, 0))
    weight_spec = pl.BlockSpec((1, d_model, width), lambda e: (e, 0, 0))
    return pl.pallas_call(
        functools.partial(hidden_kernel, cap),
        grid=(local_exp,),
        in_specs=[pl.BlockSpec(metas.shape, lambda e: (0, 0, 0))] + [tok_spec] * 4 + [weight_spec, weight_spec],
        out_specs=pl.BlockSpec((1, rows, width), lambda e: (e, 0, 0)),
        scratch_shapes=[pltpu.VMEM((rows, d_model), jnp.bfloat16)],
        out_shape=jax.ShapeDtypeStruct((local_exp, rows, width), jnp.bfloat16),
        compiler_params=params(),
        cost_estimate=cost(local_exp * rows * d_model * width * 4, local_exp * d_model * width * 4),
        name="expert_hidden",
    )(metas, *sources, w_gate, w_up)


def finish_kernel(
    cap, n_blocks, combine_hbm, peer_hbm, base_ref, hidden_ref, weight_ref, shared_ref, out_hbm,
    combine, peer, rows, total, for_tp, from_core, from_chip, from_tp, out,
    load_sem, store_sem, core_send, core_recv, chip_send, chip_recv, tp_send, tp_recv,
):
    block, group = pl.program_id(0), pl.program_id(1)
    tok_dev, cols = base_ref.shape
    core_peer, chip_peer, _, tp_peer = peers()
    load_combine = pltpu.make_async_copy(combine_hbm, combine, load_sem.at[0])
    load_peer = pltpu.make_async_copy(peer_hbm, peer, load_sem.at[1])

    def core_copy(n):
        return pltpu.make_async_remote_copy(
            src_ref=total.at[pl.ds(2, 2)], dst_ref=from_core.at[n],
            send_sem=core_send.at[n], recv_sem=core_recv.at[n], device_id=core_peer, device_id_type=MESH,
        )

    def chip_copy(n):
        return pltpu.make_async_remote_copy(
            src_ref=from_core.at[n, 1], dst_ref=from_chip.at[n],
            send_sem=chip_send.at[n], recv_sem=chip_recv.at[n], device_id=chip_peer, device_id_type=MESH,
        )

    def tp_copy(n):
        return pltpu.make_async_remote_copy(
            src_ref=for_tp.at[n], dst_ref=from_tp.at[n],
            send_sem=tp_send.at[n], recv_sem=tp_recv.at[n], device_id=tp_peer, device_id_type=MESH,
        )

    def store(n):
        here = pl.ds(pl.multiple_of(n * cols, cols), cols)
        return pltpu.make_async_copy(out.at[n], out_hbm.at[:, here], store_sem.at[n])

    def finalize(n):
        chip_copy(n).wait()
        tp_copy(n).wait()
        out[n] = (from_core[n, 0] + from_chip[n] + from_tp[n]).astype(jnp.bfloat16)
        store(n).start()

    def gated(source):
        r = rows[lax.rem(block + 1, 2), source]
        stacked = jnp.concatenate([r, r, r], axis=0)
        gates = combine[source * tok_dev : (source + 1) * tok_dev, :]
        return jnp.dot(gates, stacked, preferred_element_type=jnp.float32)

    @pl.when((block == 0) & (group == 0))
    def _():
        load_peer.start()
        load_combine.start()
        greet((core_peer, chip_peer, tp_peer))

    @pl.when(block < n_blocks)
    def _():
        results = []
        for k in range(GROUP):
            results.append(jnp.dot(hidden_ref[k], weight_ref[k], preferred_element_type=jnp.float32))
        gap = jnp.zeros((256 - GROUP * cap, cols), jnp.float32)
        place = pl.ds(pl.multiple_of(group * 256, 256), 256)
        for source in range(4):
            part = jnp.concatenate([r[source * cap : (source + 1) * cap] for r in results] + [gap], axis=0)
            rows[lax.rem(block, 2), source, place, :] = part.astype(jnp.bfloat16)

    @pl.when((block == 0) & (group == 2))
    def _():
        load_peer.wait()

    @pl.when((block == 1) & (group == 0))
    def _():
        load_combine.wait()

    @pl.when((block >= 1) & (group == 0))
    def _():
        total[2] = gated(1)

    @pl.when((block >= 1) & (group == 1))
    def _():
        total[3] = gated(3)
        core_copy(block - 1).start()

    @pl.when((block >= 1) & (group == 2))
    def _():
        total[1] = gated(2)

    @pl.when((block >= 1) & (group == 3))
    def _():
        core_copy(block - 1).wait()
        from_core[block - 1, 1] += total[1]
        chip_copy(block - 1).start()
        total[0] = gated(0) + base_ref[...]
        from_core[block - 1, 0] += total[0]

    @pl.when((block < n_blocks) & (group == 4))
    def _():
        for_tp[block] = jnp.dot(peer[...], shared_ref[...], preferred_element_type=jnp.float32)
        tp_copy(block).start()

    @pl.when((block >= 4) & (group == 4))
    def _():
        finalize(block - 4)

    @pl.when((block == n_blocks) & (group == 4))
    def _():
        for n in range(n_blocks - 3, n_blocks):
            finalize(n)
        for n in range(n_blocks):
            store(n).wait()


def finish(hidden, combine, base, peer_hidden, w_down, shared_down_w):
    local_exp, n_rows, width = hidden.shape
    n_groups = local_exp // GROUP
    tok_dev, d_model = base.shape
    shared_width = peer_hidden.shape[1]
    cols = d_model // COL_BLOCKS
    last_block, last_group = COL_BLOCKS - 1, n_groups - 1
    sems = pltpu.SemaphoreType.DMA((COL_BLOCKS,))
    blocks = (COL_BLOCKS, tok_dev, cols)

    def group_of(n, g):
        return jnp.where(n > last_block, last_group, g)

    return pl.pallas_call(
        functools.partial(finish_kernel, n_rows // 4, COL_BLOCKS),
        grid=(COL_BLOCKS + 1, n_groups),
        out_shape=jax.ShapeDtypeStruct((tok_dev, d_model), jnp.bfloat16),
        in_specs=[
            ANY,
            ANY,
            pl.BlockSpec((tok_dev, cols), lambda n, g: (0, jnp.maximum(n - 1, 0))),
            pl.BlockSpec((GROUP, n_rows, width), lambda n, g: (group_of(n, g), 0, 0)),
            pl.BlockSpec((GROUP, width, cols), lambda n, g: (group_of(n, g), 0, jnp.minimum(n, last_block))),
            pl.BlockSpec((shared_width, cols), lambda n, g: (0, jnp.minimum(n, last_block))),
        ],
        out_specs=ANY,
        scratch_shapes=[
            pltpu.VMEM(combine.shape, jnp.bfloat16),
            pltpu.VMEM(peer_hidden.shape, jnp.bfloat16),
            pltpu.VMEM((2, 4, n_groups * 256, cols), jnp.bfloat16),
            pltpu.VMEM((4, tok_dev, cols), jnp.float32),
            pltpu.VMEM(blocks, jnp.float32),
            pltpu.VMEM((COL_BLOCKS, 2, tok_dev, cols), jnp.float32),
            pltpu.VMEM(blocks, jnp.float32),
            pltpu.VMEM(blocks, jnp.float32),
            pltpu.VMEM(blocks, jnp.bfloat16),
            pltpu.SemaphoreType.DMA((2,)),
            sems, sems, sems, sems, sems, sems, sems,
        ],
        compiler_params=pltpu.CompilerParams(
            collective_id=0, has_side_effects=True, vmem_limit_bytes=67043328, dimension_semantics=("arbitrary", "arbitrary")
        ),
        cost_estimate=cost(2 * d_model * local_exp * (n_rows * width + 4 * tok_dev * 256), 2 * local_exp * width * d_model),
        name="finish",
    )(combine, peer_hidden, base, hidden, w_down, shared_down_w)


def solution(mesh):
    ep_size = mesh.shape["ep"]
    row_spec = P(("dp", "ep", "tp"), None)
    expert_spec = P("ep", None, None)

    def local_layer(tokens, expert_ids, gates, slots, shared_w1, shared_w3, shared_w2, expert_w1, expert_w3, expert_w2):
        tok_dev, d_model = tokens.shape
        top_k = expert_ids.shape[1]
        local_exp = expert_w1.shape[0]
        cap = capacity_rows(tok_dev, top_k, local_exp * ep_size)
        code = jnp.where(slots >= 0, expert_ids * cap + slots, -1)
        meta = jnp.concatenate([code.astype(jnp.float32).T, gates.T], axis=0)
        metas, tok_core, tok_chip, tok_both, combine, base, peer_hidden = start(meta, tokens, shared_w1, shared_w3, shared_w2, cap, local_exp)
        hidden = expert_hidden(metas, (tokens, tok_core, tok_chip, tok_both), expert_w1, expert_w3, cap)
        return finish(hidden, combine, base, peer_hidden, expert_w2, shared_w2)

    return jax.shard_map(local_layer, mesh=mesh, in_specs=(row_spec, row_spec, row_spec, row_spec, P(None, "tp"), P(None, "tp"), P("tp", None), expert_spec, expert_spec, expert_spec), out_specs=row_spec, check_vma=False)
```

```python
import functools

import jax
import jax.numpy as jnp
from jax import lax
from jax.experimental import pallas as pl
from jax.experimental.pallas import tpu as pltpu
from jax.sharding import PartitionSpec as P
import numpy as np

COL_BLOCKS = 8
GROUP = 5
BATCH = 4
FEW_SLOTS = 48
SPAN = 512
CHUNK = 128
MESH = pl.DeviceIdType.MESH
GATE_MAX = 3.3895313892515355e38


def capacity_rows(tok_dev, top_k, n_exp):
    return 8 * max(1, (2 * tok_dev * top_k + 8 * n_exp - 1) // (8 * n_exp))


ANY = pl.BlockSpec(memory_space=pl.ANY)


def params():
    return pltpu.CompilerParams(vmem_limit_bytes=62 * 2**20)


def cost(flops, nbytes):
    return pl.CostEstimate(flops=flops, bytes_accessed=nbytes, transcendentals=0)


def peers():
    dp, tp, me = lax.axis_index("dp"), lax.axis_index("tp"), lax.axis_index("ep")
    core = me + 1 - 2 * lax.rem(me, 2)
    chip = lax.rem(me + 2, 4)
    both = lax.rem(core + 2, 4)
    return (dp, tp, core), (dp, tp, chip), (dp, tp, both), (dp, 1 - tp, me)


def greet(devices):
    barrier = pltpu.get_barrier_semaphore()
    for device in devices:
        pl.semaphore_signal(barrier, inc=1, device_id=device, device_id_type=MESH)
    pl.semaphore_wait(barrier, len(devices))


def lane_tables(cap, local_exp):
    span = 128 * ((GROUP * cap + 127) // 128)
    lane = np.arange(local_exp // GROUP * span)
    place = lane % span
    expert = np.where(place < GROUP * cap, lane // span * GROUP + place // cap, -1)
    owner = (np.arange(128)[:, None] == expert[None, :]).astype(np.float32)
    slot = np.where(expert >= 0, place % cap, -1).astype(np.float32)
    return span, jnp.asarray(owner, jnp.bfloat16), jnp.asarray(np.tile(slot, (8, 1)))


def combine_chunk(cap, local_exp, meta, owner_ref, slot_ref, out_ref):
    top_k = meta.shape[0] // 2
    cols = meta.T
    lane = lax.broadcasted_iota(jnp.int32, (CHUNK, 128), 1)
    base = ((lane + lax.axis_index("ep") * local_exp) * cap).astype(jnp.float32)
    slot_of = jnp.full(base.shape, -1024.0, jnp.float32)
    gate = jnp.zeros(base.shape, jnp.float32)
    for j in range(top_k):
        offset = cols[:, j : j + 1] - base
        inside = (offset >= 0.0) & (offset < float(cap)) & (lane < local_exp)
        slot_of = jnp.where(inside, offset, slot_of)
        gate = jnp.where(inside, cols[:, top_k + j : top_k + j + 1], gate)
    high = jnp.minimum(gate, GATE_MAX).astype(jnp.bfloat16).astype(jnp.float32)
    rest = gate - high
    middle = rest.astype(jnp.bfloat16).astype(jnp.float32)
    table = jnp.concatenate([slot_of, high, middle, rest - middle], axis=0).astype(jnp.bfloat16)
    spread = jnp.dot(table, owner_ref[...], preferred_element_type=jnp.float32)
    hit = spread[:CHUNK] == slot_ref[0:1, :]
    depth = spread.shape[1]
    for i in range(3):
        out_ref[:, i * depth : (i + 1) * depth] = jnp.where(hit, spread[(i + 1) * CHUNK : (i + 2) * CHUNK], 0.0).astype(jnp.bfloat16)


def start_kernel(
    cap, local_exp, meta_ref, owner_ref, slot_ref, tok_hbm, w_gate_hbm, w_up_hbm, w_down_hbm,
    metas, tok_core, tok_chip, tok_both, combine_hbm, base_hbm, peer_hidden,
    own, other, own_hidden, load_sem, send_sem, recv_sem,
):
    core, chip, both, tp = peers()
    tok_dev, d_model = own.shape
    width = peer_hidden.shape[1]

    def remote(src, dst, device, i):
        return pltpu.make_async_remote_copy(
            src_ref=src, dst_ref=dst, send_sem=send_sem.at[i], recv_sem=recv_sem.at[i], device_id=device, device_id_type=MESH
        )

    load = pltpu.make_async_copy(tok_hbm, own, load_sem)
    load.start()
    greet((core, chip, both, tp))
    meta_copies = [remote(meta_ref, metas.at[i + 1], device, i) for i, device in enumerate((core, chip, both))]
    for copy in meta_copies:
        copy.start()
    to_chip = remote(tok_hbm, tok_chip, chip, 3)
    to_tp = remote(tok_hbm, other, tp, 4)
    to_core = remote(tok_hbm, tok_core, core, 5)
    onward = remote(tok_chip, tok_both, core, 6)
    for copy in (to_chip, to_tp, to_core):
        copy.start()
    metas[0] = meta_ref[...]
    for copy in meta_copies:
        copy.wait()

    per_source = tok_dev // CHUNK

    def write_combine(index, out_ref):
        i = index.index[0]
        here = pl.ds(pl.multiple_of(lax.rem(i, per_source) * CHUNK, CHUNK), CHUNK)
        combine_chunk(cap, local_exp, metas[i // per_source, :, here], owner_ref, slot_ref, out_ref)

    pltpu.emit_pipeline(
        write_combine,
        grid=(4 * per_source,),
        out_specs=[pl.BlockSpec((CHUNK, combine_hbm.shape[1]), lambda i: (i, 0))],
        _explicit_indices=True,
    )(combine_hbm)

    def hidden_of(rows, result):
        def part(first, step, count):
            def body(index, gate_w_ref, up_w_ref):
                gate_pre = jnp.dot(rows[...], gate_w_ref[...], preferred_element_type=jnp.float32)
                up_pre = jnp.dot(rows[...], up_w_ref[...], preferred_element_type=jnp.float32)
                here = pl.ds(pl.multiple_of((first + index.index[0]) * step, step), step)
                result[:, here] = (jax.nn.silu(gate_pre) * up_pre).astype(jnp.bfloat16)

            spec = pl.BlockSpec((d_model, step), lambda i: (0, first + i))
            pltpu.emit_pipeline(body, grid=(count,), in_specs=[spec, spec], _explicit_indices=True)(w_gate_hbm, w_up_hbm)

        part(0, 256, width // 256)

    load.wait()
    hidden_of(own, own_hidden)

    def down(index, weight_ref, out_ref):
        here = pl.ds(pl.multiple_of(index.index[0] * 512, 512), 512)
        result = jnp.dot(own_hidden[...], weight_ref[...], preferred_element_type=jnp.float32)
        out_ref[...] = own[:, here].astype(jnp.float32) + result

    pltpu.emit_pipeline(
        down,
        grid=(d_model // 512,),
        in_specs=[pl.BlockSpec((width, 512), lambda i: (0, i))],
        out_specs=[pl.BlockSpec((tok_dev, 512), lambda i: (0, i))],
        _explicit_indices=True,
    )(w_down_hbm, base_hbm)

    to_chip.wait()
    onward.start()
    to_tp.wait()
    hidden_of(other, peer_hidden)
    to_core.wait()
    onward.wait()


def start(meta, owner, slot, tokens, w_gate, w_up, w_down, cap, local_exp):
    tok_dev, d_model = tokens.shape
    width = w_gate.shape[1]
    vmem = pl.BlockSpec(memory_space=pltpu.VMEM)
    tok_shape = jax.ShapeDtypeStruct((tok_dev, d_model), jnp.bfloat16)
    return pl.pallas_call(
        functools.partial(start_kernel, cap, local_exp),
        out_shape=[
            jax.ShapeDtypeStruct((4,) + meta.shape, jnp.float32),
            tok_shape, tok_shape, tok_shape,
            jax.ShapeDtypeStruct((4 * tok_dev, 3 * owner.shape[1]), jnp.bfloat16),
            jax.ShapeDtypeStruct((tok_dev, d_model), jnp.float32),
            jax.ShapeDtypeStruct((tok_dev, width), jnp.bfloat16),
        ],
        in_specs=[vmem, vmem, vmem, ANY, ANY, ANY, ANY],
        out_specs=[vmem, ANY, ANY, ANY, ANY, ANY, vmem],
        scratch_shapes=[
            pltpu.VMEM((tok_dev, d_model), jnp.bfloat16),
            pltpu.VMEM((tok_dev, d_model), jnp.bfloat16),
            pltpu.VMEM((tok_dev, width), jnp.bfloat16),
            pltpu.SemaphoreType.DMA,
            pltpu.SemaphoreType.DMA((7,)),
            pltpu.SemaphoreType.DMA((7,)),
        ],
        compiler_params=pltpu.CompilerParams(collective_id=1, has_side_effects=True, vmem_limit_bytes=67043328),
        cost_estimate=cost(10 * tok_dev * d_model * width, 10 * d_model * width),
        name="start",
    )(meta, owner, slot, tokens, w_gate, w_up, w_down)


def hidden_kernel(cap, pitch, meta_ref, *refs):
    tok_hbm, (gate_hbm, up_hbm, out_ref, tok, rows, gate_w, up_w, tok_sem, gate_sem, up_sem) = refs[:4], refs[4:]
    e = pl.program_id(0)
    n_exp = pl.num_programs(0)
    width = out_ref.shape[2]
    d_model = tok.shape[2]
    top_k = meta_ref.shape[1] // 2
    spans = [slice(start, min(start + SPAN, width)) for start in range(0, width, SPAN)]
    now = lax.rem(e, 2)
    first = (lax.axis_index("ep") * n_exp) * cap

    def load_tok(s):
        return pltpu.make_async_copy(tok_hbm[s], tok.at[s], tok_sem.at[s])

    def load(i):
        slot = lax.rem(i, 2)
        return (
            pltpu.make_async_copy(gate_hbm.at[i], gate_w.at[slot], gate_sem.at[slot]),
            pltpu.make_async_copy(up_hbm.at[i], up_w.at[slot], up_sem.at[slot]),
        )

    def pick_rows(batch, source):
        slot = meta_ref[source, :top_k].astype(jnp.int32) - (first + batch * (BATCH * cap))
        row = lax.broadcasted_iota(jnp.int32, (BATCH * cap, slot.shape[1]), 0)
        hit = row == slot[0:1, :]
        for j in range(1, top_k):
            hit = hit | (row == slot[j : j + 1, :])
        pick = jnp.where(hit, 1.0, 0.0).astype(jnp.bfloat16)
        place = pl.ds(pl.multiple_of(source * pitch, pitch), cap)
        for start in range(0, d_model, 512):
            picked = jnp.dot(pick, tok[source, :, start : start + 512], preferred_element_type=jnp.float32)
            for k in range(BATCH):
                part = picked[k * cap : (k + 1) * cap].astype(jnp.bfloat16)
                rows[lax.rem(batch, 2), k, place, start : start + 512] = part

    @pl.when(e == 0)
    def _():
        for s in range(4):
            load_tok(s).start()
        for copy in load(0):
            copy.start()
        for s in range(4):
            load_tok(s).wait()
        pl.loop(0, 4)(lambda s: pick_rows(0, s))

    @pl.when(e + 1 < n_exp)
    def _():
        for copy in load(e + 1):
            copy.start()

    @pl.when(e // BATCH < (n_exp - 1) // BATCH)
    def _():
        pick_rows(e // BATCH + 1, lax.rem(e, BATCH))

    for copy in load(e):
        copy.wait()

    mine = [meta_ref[source, :top_k].astype(jnp.int32) - (first + e * cap) for source in range(4)]
    last = jnp.max(jnp.stack([jnp.where(slot < cap, slot, -1) for slot in mine]))
    batch, k = lax.rem(e // BATCH, 2), lax.rem(e, BATCH)

    def swiglu_cols(x, cols):
        gate_pre = jnp.dot(x, gate_w[now, :, cols], preferred_element_type=jnp.float32)
        up_pre = jnp.dot(x, up_w[now, :, cols], preferred_element_type=jnp.float32)
        return jax.nn.silu(gate_pre) * up_pre

    @pl.when(last < FEW_SLOTS)
    def _():
        x = jnp.concatenate([rows[batch, k, s * pitch : s * pitch + FEW_SLOTS] for s in range(4)], axis=0)
        for cols in spans:
            hidden = swiglu_cols(x, cols)
            gap = jnp.zeros((cap - FEW_SLOTS, hidden.shape[1]), jnp.float32)
            pieces = []
            for s in range(4):
                pieces += [hidden[s * FEW_SLOTS : (s + 1) * FEW_SLOTS], gap]
            out_ref[0, :, cols] = jnp.concatenate(pieces, axis=0).astype(jnp.bfloat16)

    @pl.when(last >= FEW_SLOTS)
    def _():
        x = rows[batch, k]
        for cols in spans:
            hidden = swiglu_cols(x, cols)
            pieces = [hidden[s * pitch : s * pitch + cap] for s in range(4)]
            out_ref[0, :, cols] = jnp.concatenate(pieces, axis=0).astype(jnp.bfloat16)


def expert_hidden(metas, sources, w_gate, w_up, cap):
    local_exp, d_model, width = w_gate.shape
    tok_dev = sources[0].shape[0]
    pitch = 16 * ((cap + 15) // 16)
    rows = 4 * cap
    return pl.pallas_call(
        functools.partial(hidden_kernel, cap, pitch),
        grid=(local_exp,),
        in_specs=[pl.BlockSpec(metas.shape, lambda e: (0, 0, 0))] + [ANY] * 6,
        out_specs=pl.BlockSpec((1, rows, width), lambda e: (e, 0, 0)),
        scratch_shapes=[
            pltpu.VMEM((4, tok_dev, d_model), jnp.bfloat16),
            pltpu.VMEM((2, BATCH, 4 * pitch, d_model), jnp.bfloat16),
            pltpu.VMEM((2, d_model, width), jnp.bfloat16),
            pltpu.VMEM((2, d_model, width), jnp.bfloat16),
            pltpu.SemaphoreType.DMA((4,)),
            pltpu.SemaphoreType.DMA((2,)),
            pltpu.SemaphoreType.DMA((2,)),
        ],
        out_shape=jax.ShapeDtypeStruct((local_exp, rows, width), jnp.bfloat16),
        compiler_params=params(),
        cost_estimate=cost(local_exp * rows * d_model * width * 4, local_exp * d_model * width * 4),
        name="expert_hidden",
    )(metas, *sources, w_gate, w_up)


def finish_kernel(
    cap, span, n_blocks, combine_hbm, peer_hbm, hidden_hbm, base_ref, weight_ref, shared_ref, out_hbm,
    combine, peer, hidden, rows, kept, given, for_tp, from_core, from_chip, from_tp, out,
    peer_sem, combine_sem, hidden_sem, store_sem, core_send, core_recv, chip_send, chip_recv, tp_send, tp_recv,
):
    step, group = pl.program_id(0), pl.program_id(1)
    n_steps = 2 * n_blocks
    tok_dev, cols = base_ref.shape
    core_peer, chip_peer, _, tp_peer = peers()
    load_peer = pltpu.make_async_copy(peer_hbm, peer, peer_sem)

    def load_combine(near, half):
        source = half if near else 2 + half
        return pltpu.make_async_copy(combine_hbm.at[pl.ds(source * tok_dev, tok_dev)], combine.at[half], combine_sem.at[half])

    def load_hidden(near, g):
        experts = pl.ds(g * GROUP, GROUP)
        source = pl.ds(0 if near else 2 * cap, 2 * cap)
        return pltpu.make_async_copy(hidden_hbm.at[experts, source], hidden.at[experts], hidden_sem.at[g])

    def core_copy(i):
        return pltpu.make_async_remote_copy(
            src_ref=given, dst_ref=from_core.at[i],
            send_sem=core_send.at[i], recv_sem=core_recv.at[i], device_id=core_peer, device_id_type=MESH,
        )

    def chip_copy(n):
        return pltpu.make_async_remote_copy(
            src_ref=from_core.at[n], dst_ref=from_chip.at[n],
            send_sem=chip_send.at[n], recv_sem=chip_recv.at[n], device_id=chip_peer, device_id_type=MESH,
        )

    def tp_copy(n):
        return pltpu.make_async_remote_copy(
            src_ref=for_tp.at[n], dst_ref=from_tp.at[n],
            send_sem=tp_send.at[n], recv_sem=tp_recv.at[n], device_id=tp_peer, device_id_type=MESH,
        )

    def store(n):
        here = pl.ds(pl.multiple_of(n * cols, cols), cols)
        return pltpu.make_async_copy(out.at[n], out_hbm.at[:, here], store_sem.at[n])

    def finalize(n):
        chip_copy(n).wait()
        tp_copy(n).wait()
        out[n] = (from_core[n_blocks + n] + from_chip[n] + from_tp[n]).astype(jnp.bfloat16)
        store(n).start()

    def gated(half):
        r = rows[lax.rem(step + 1, 2), half]
        return jnp.dot(combine[half], jnp.concatenate([r, r, r], axis=0), preferred_element_type=jnp.float32)

    @pl.when((step == 0) & (group == 0))
    def _():
        for g in range(hidden_sem.shape[0]):
            load_hidden(False, g).start()
        load_peer.start()
        for half in (1, 0):
            load_combine(False, half).start()
        greet((core_peer, chip_peer, tp_peer))

    @pl.when(step == 0)
    def _():
        load_hidden(False, group).wait()

    @pl.when(step == n_blocks)
    def _():
        load_hidden(True, group).wait()

    @pl.when(step < n_steps)
    def _():
        results = []
        for k in range(GROUP):
            results.append(jnp.dot(hidden[group * GROUP + k], weight_ref[k], preferred_element_type=jnp.float32))
        gap = jnp.zeros((span - GROUP * cap, cols), jnp.float32)
        place = pl.ds(pl.multiple_of(group * span, span), span)
        for half in range(2):
            part = jnp.concatenate([r[half * cap : (half + 1) * cap] for r in results] + [gap], axis=0)
            rows[lax.rem(step, 2), half, place, :] = part.astype(jnp.bfloat16)

    @pl.when(step == n_blocks - 1)
    def _():
        load_hidden(True, group).start()

    for near in (False, True):
        start = n_blocks + 1 if near else 1

        @pl.when((step == start) & (group < 2))
        def _():
            load_combine(near, 1 - group).wait()

    @pl.when((step >= 1) & (group == 0))
    def _():
        given[...] = gated(1)
        core_copy(step - 1).start()

    @pl.when((step >= 1) & (group == 1))
    def _():
        kept[...] = gated(0)

    @pl.when((step == n_blocks) & (group < 2))
    def _():
        load_combine(True, 1 - group).start()

    @pl.when((step >= 1) & (group == 2))
    def _():
        core_copy(step - 1).wait()
        from_core[step - 1] += kept[...]

    @pl.when((step >= 1) & (step <= n_blocks) & (group == 2))
    def _():
        chip_copy(step - 1).start()

    @pl.when((step > n_blocks) & (group == 2))
    def _():
        from_core[step - 1] += base_ref[...]

    @pl.when((step == 0) & (group == 2))
    def _():
        load_peer.wait()

    @pl.when((step < n_blocks) & (group == 2))
    def _():
        for_tp[step] = jnp.dot(peer[...], shared_ref[...], preferred_element_type=jnp.float32)
        tp_copy(step).start()

    @pl.when((step > n_blocks) & (step <= n_blocks + 4) & (group == 2))
    def _():
        finalize(step - 1 - n_blocks)

    @pl.when((step == n_steps) & (group == 2))
    def _():
        for n in range(4, n_blocks):
            finalize(n)
        for n in range(n_blocks):
            store(n).wait()


def finish(hidden, combine, base, peer_hidden, w_down, shared_down_w):
    local_exp, n_rows, width = hidden.shape
    n_groups = local_exp // GROUP
    cap = n_rows // 4
    depth = combine.shape[1]
    tok_dev, d_model = base.shape
    shared_width = peer_hidden.shape[1]
    cols = d_model // COL_BLOCKS
    sems = pltpu.SemaphoreType.DMA((COL_BLOCKS,))
    two_sems = pltpu.SemaphoreType.DMA((2 * COL_BLOCKS,))
    blocks = (COL_BLOCKS, tok_dev, cols)

    def weight_map(i, g):
        running = i < 2 * COL_BLOCKS
        return jnp.where(running, g, n_groups - 1), 0, jnp.where(running, lax.rem(i, COL_BLOCKS), COL_BLOCKS - 1)

    return pl.pallas_call(
        functools.partial(finish_kernel, cap, depth // 3 // n_groups, COL_BLOCKS),
        grid=(2 * COL_BLOCKS + 1, n_groups),
        out_shape=jax.ShapeDtypeStruct((tok_dev, d_model), jnp.bfloat16),
        in_specs=[
            ANY,
            ANY,
            ANY,
            pl.BlockSpec((tok_dev, cols), lambda i, g: (0, jnp.maximum(i - COL_BLOCKS - 1, 0))),
            pl.BlockSpec((GROUP, width, cols), weight_map),
            pl.BlockSpec((shared_width, cols), lambda i, g: (0, jnp.minimum(i, COL_BLOCKS - 1))),
        ],
        out_specs=ANY,
        scratch_shapes=[
            pltpu.VMEM((2, tok_dev, depth), jnp.bfloat16),
            pltpu.VMEM(peer_hidden.shape, jnp.bfloat16),
            pltpu.VMEM((local_exp, 2 * cap, width), jnp.bfloat16),
            pltpu.VMEM((2, 2, depth // 3, cols), jnp.bfloat16),
            pltpu.VMEM((tok_dev, cols), jnp.float32),
            pltpu.VMEM((tok_dev, cols), jnp.float32),
            pltpu.VMEM(blocks, jnp.float32),
            pltpu.VMEM((2 * COL_BLOCKS, tok_dev, cols), jnp.float32),
            pltpu.VMEM(blocks, jnp.float32),
            pltpu.VMEM(blocks, jnp.float32),
            pltpu.VMEM(blocks, jnp.bfloat16),
            pltpu.SemaphoreType.DMA,
            pltpu.SemaphoreType.DMA((2,)),
            pltpu.SemaphoreType.DMA((n_groups,)),
            sems, two_sems, two_sems, sems, sems, sems, sems,
        ],
        compiler_params=pltpu.CompilerParams(
            collective_id=0, has_side_effects=True, vmem_limit_bytes=67043328, dimension_semantics=("arbitrary", "arbitrary")
        ),
        cost_estimate=cost(2 * d_model * local_exp * (n_rows * width + 4 * tok_dev * 256), 2 * local_exp * width * d_model),
        name="finish",
    )(combine, peer_hidden, hidden, base, w_down, shared_down_w)


def solution(mesh):
    ep_size = mesh.shape["ep"]
    row_spec = P(("dp", "ep", "tp"), None)
    expert_spec = P("ep", None, None)

    def local_layer(tokens, expert_ids, gates, slots, shared_w1, shared_w3, shared_w2, expert_w1, expert_w3, expert_w2):
        tok_dev, d_model = tokens.shape
        top_k = expert_ids.shape[1]
        local_exp = expert_w1.shape[0]
        cap = capacity_rows(tok_dev, top_k, local_exp * ep_size)
        code = jnp.where(slots >= 0, expert_ids * cap + slots, -1)
        meta = jnp.concatenate([code.astype(jnp.float32).T, gates.T], axis=0)
        _, owner, slot = lane_tables(cap, local_exp)
        metas, tok_core, tok_chip, tok_both, combine, base, peer_hidden = start(meta, owner, slot, tokens, shared_w1, shared_w3, shared_w2, cap, local_exp)
        hidden = expert_hidden(metas, (tokens, tok_core, tok_chip, tok_both), expert_w1, expert_w3, cap)
        return finish(hidden, combine, base, peer_hidden, expert_w2, shared_w2)

    return jax.shard_map(local_layer, mesh=mesh, in_specs=(row_spec, row_spec, row_spec, row_spec, P(None, "tp"), P(None, "tp"), P("tp", None), expert_spec, expert_spec, expert_spec), out_specs=row_spec, check_vma=False)
```

```python
import functools

import jax
import jax.numpy as jnp
from jax import lax
from jax.experimental import pallas as pl
from jax.experimental.pallas import tpu as pltpu
from jax.sharding import PartitionSpec as P
import numpy as np

COL_BLOCKS = 8
GROUP = 5
BATCH = 4
BUFFERS = 3
FEW_SLOTS = 48
SPAN = 512
CHUNK = 128
MESH = pl.DeviceIdType.MESH
GATE_MAX = 3.3895313892515355e38


def capacity_rows(tok_dev, top_k, n_exp):
    return 8 * max(1, (2 * tok_dev * top_k + 8 * n_exp - 1) // (8 * n_exp))


ANY = pl.BlockSpec(memory_space=pl.ANY)


def params():
    return pltpu.CompilerParams(vmem_limit_bytes=62 * 2**20)


def cost(flops, nbytes):
    return pl.CostEstimate(flops=flops, bytes_accessed=nbytes, transcendentals=0)


def peers():
    dp, tp, me = lax.axis_index("dp"), lax.axis_index("tp"), lax.axis_index("ep")
    core = me + 1 - 2 * lax.rem(me, 2)
    chip = lax.rem(me + 2, 4)
    both = lax.rem(core + 2, 4)
    return (dp, tp, core), (dp, tp, chip), (dp, tp, both), (dp, 1 - tp, me)


def greet(devices):
    barrier = pltpu.get_barrier_semaphore()
    for device in devices:
        pl.semaphore_signal(barrier, inc=1, device_id=device, device_id_type=MESH)
    pl.semaphore_wait(barrier, len(devices))


def lane_tables(cap, local_exp):
    span = 128 * ((GROUP * cap + 127) // 128)
    lane = np.arange(local_exp // GROUP * span)
    place = lane % span
    expert = np.where(place < GROUP * cap, lane // span * GROUP + place // cap, -1)
    owner = (np.arange(128)[:, None] == expert[None, :]).astype(np.float32)
    slot = np.where(expert >= 0, place % cap, -1).astype(np.float32)
    return span, jnp.asarray(owner, jnp.bfloat16), jnp.asarray(np.tile(slot, (8, 1)))


def combine_chunk(cap, local_exp, meta, owner_ref, slot_ref, out_ref):
    top_k = meta.shape[0] // 2
    cols = meta.T
    lane = lax.broadcasted_iota(jnp.int32, (CHUNK, 128), 1)
    base = ((lane + lax.axis_index("ep") * local_exp) * cap).astype(jnp.float32)
    slot_of = jnp.full(base.shape, -1024.0, jnp.float32)
    gate = jnp.zeros(base.shape, jnp.float32)
    for j in range(top_k):
        offset = cols[:, j : j + 1] - base
        inside = (offset >= 0.0) & (offset < float(cap)) & (lane < local_exp)
        slot_of = jnp.where(inside, offset, slot_of)
        gate = jnp.where(inside, cols[:, top_k + j : top_k + j + 1], gate)
    high = jnp.minimum(gate, GATE_MAX).astype(jnp.bfloat16).astype(jnp.float32)
    rest = gate - high
    middle = rest.astype(jnp.bfloat16).astype(jnp.float32)
    table = jnp.concatenate([slot_of, high, middle, rest - middle], axis=0).astype(jnp.bfloat16)
    spread = jnp.dot(table, owner_ref[...], preferred_element_type=jnp.float32)
    hit = spread[:CHUNK] == slot_ref[0:1, :]
    n_groups = out_ref.shape[0]
    span = spread.shape[1] // n_groups
    for i in range(3):
        value = jnp.where(hit, spread[(i + 1) * CHUNK : (i + 2) * CHUNK], 0.0).astype(jnp.bfloat16)
        for g in range(n_groups):
            out_ref[g, :, i * span : (i + 1) * span] = value[:, g * span : (g + 1) * span]


def start_kernel(
    cap, local_exp, meta_ref, owner_ref, slot_ref, tok_hbm, w_gate_hbm, w_up_hbm, w_down_hbm,
    metas, tok_core, tok_chip, tok_both, combine_hbm, base_hbm, peer_hbm,
    own, other, own_hidden, peer_hidden, base, w_gate, w_up, w_down,
    load_sem, store_sem, peer_sem, send_sem, recv_sem,
):
    core, chip, both, tp = peers()
    tok_dev, d_model = own.shape
    width = peer_hidden.shape[1]

    def remote(src, dst, device, i):
        return pltpu.make_async_remote_copy(
            src_ref=src, dst_ref=dst, send_sem=send_sem.at[i], recv_sem=recv_sem.at[i], device_id=device, device_id_type=MESH
        )

    greet((core, chip, both, tp))
    meta_copies = [remote(meta_ref, metas.at[i + 1], device, i) for i, device in enumerate((core, chip, both))]
    for copy in meta_copies:
        copy.start()
    to_chip = remote(tok_hbm, tok_chip, chip, 3)
    to_core = remote(tok_hbm, tok_core, core, 4)
    onward = remote(tok_chip, tok_both, core, 5)
    parts = [pl.ds(0, tok_dev // 2), pl.ds(tok_dev // 2, tok_dev // 4), pl.ds(tok_dev // 4 * 3, tok_dev // 4)]
    to_tp = [remote(tok_hbm.at[part], other.at[part], tp, 6 + i) for i, part in enumerate(parts)]
    to_chip.start()
    for copy in to_tp:
        copy.start()
    to_core.start()
    pairs = ((tok_hbm, own), (w_gate_hbm, w_gate), (w_up_hbm, w_up), (w_down_hbm, w_down))
    loads = [pltpu.make_async_copy(src, dst, load_sem.at[i]) for i, (src, dst) in enumerate(pairs)]
    for load in loads:
        load.start()
    metas[0] = meta_ref[...]
    for copy in meta_copies:
        copy.wait()

    per_source = tok_dev // CHUNK

    def write_combine(index, out_ref):
        i = index.index[0]
        here = pl.ds(pl.multiple_of(lax.rem(i, per_source) * CHUNK, CHUNK), CHUNK)
        combine_chunk(cap, local_exp, metas[i // per_source, :, here], owner_ref, slot_ref, out_ref)

    n_groups, _, depth = combine_hbm.shape
    pltpu.emit_pipeline(
        write_combine,
        grid=(4 * per_source,),
        out_specs=[pl.BlockSpec((n_groups, CHUNK, depth), lambda i: (0, i, 0))],
        _explicit_indices=True,
    )(combine_hbm)

    def hidden_of(rows, result, here):
        def cols_of(cols):
            gate_pre = jnp.dot(rows[here], w_gate[:, cols], preferred_element_type=jnp.float32)
            up_pre = jnp.dot(rows[here], w_up[:, cols], preferred_element_type=jnp.float32)
            result[here, cols] = (jax.nn.silu(gate_pre) * up_pre).astype(jnp.bfloat16)

        whole = width // SPAN * SPAN

        @pl.loop(0, width // SPAN)
        def _(i):
            cols_of(pl.ds(pl.multiple_of(i * SPAN, SPAN), SPAN))

        if whole < width:
            cols_of(pl.ds(whole, width - whole))

    for load in loads[:3]:
        load.wait()
    hidden_of(own, own_hidden, pl.ds(0, tok_dev))

    def store_peer(i):
        return pltpu.make_async_copy(peer_hidden.at[parts[i]], peer_hbm.at[parts[i]], peer_sem.at[i])

    to_tp[0].wait()
    hidden_of(other, peer_hidden, parts[0])
    store_peer(0).start()
    loads[3].wait()

    @pl.loop(0, d_model // SPAN)
    def _(i):
        cols = pl.ds(pl.multiple_of(i * SPAN, SPAN), SPAN)
        down = jnp.dot(own_hidden[...], w_down[:, cols], preferred_element_type=jnp.float32)
        base[:, cols] = own[:, cols].astype(jnp.float32) + down

    store = pltpu.make_async_copy(base, base_hbm, store_sem)
    store.start()
    to_tp[1].wait()
    hidden_of(other, peer_hidden, parts[1])
    store_peer(1).start()
    to_chip.wait()
    onward.start()
    to_tp[2].wait()
    hidden_of(other, peer_hidden, parts[2])
    store_peer(2).start()
    for i in range(3):
        store_peer(i).wait()
    store.wait()
    to_core.wait()
    onward.wait()


def start(meta, owner, slot, tokens, w_gate, w_up, w_down, cap, local_exp):
    tok_dev, d_model = tokens.shape
    width = w_gate.shape[1]
    n_groups = local_exp // GROUP
    vmem = pl.BlockSpec(memory_space=pltpu.VMEM)
    tok_shape = jax.ShapeDtypeStruct((tok_dev, d_model), jnp.bfloat16)
    return pl.pallas_call(
        functools.partial(start_kernel, cap, local_exp),
        out_shape=[
            jax.ShapeDtypeStruct((4,) + meta.shape, jnp.float32),
            tok_shape, tok_shape, tok_shape,
            jax.ShapeDtypeStruct((n_groups, 4 * tok_dev, 3 * owner.shape[1] // n_groups), jnp.bfloat16),
            jax.ShapeDtypeStruct((tok_dev, d_model), jnp.float32),
            jax.ShapeDtypeStruct((tok_dev, width), jnp.bfloat16),
        ],
        in_specs=[vmem, vmem, vmem, ANY, ANY, ANY, ANY],
        out_specs=[vmem, ANY, ANY, ANY, ANY, ANY, ANY],
        scratch_shapes=[
            pltpu.VMEM((tok_dev, d_model), jnp.bfloat16),
            pltpu.VMEM((tok_dev, d_model), jnp.bfloat16),
            pltpu.VMEM((tok_dev, width), jnp.bfloat16),
            pltpu.VMEM((tok_dev, width), jnp.bfloat16),
            pltpu.VMEM((tok_dev, d_model), jnp.float32),
            pltpu.VMEM((d_model, width), jnp.bfloat16),
            pltpu.VMEM((d_model, width), jnp.bfloat16),
            pltpu.VMEM((width, d_model), jnp.bfloat16),
            pltpu.SemaphoreType.DMA((4,)),
            pltpu.SemaphoreType.DMA,
            pltpu.SemaphoreType.DMA((3,)),
            pltpu.SemaphoreType.DMA((9,)),
            pltpu.SemaphoreType.DMA((9,)),
        ],
        compiler_params=pltpu.CompilerParams(collective_id=1, has_side_effects=True, vmem_limit_bytes=67043328),
        cost_estimate=cost(10 * tok_dev * d_model * width, 10 * d_model * width),
        name="start",
    )(meta, owner, slot, tokens, w_gate, w_up, w_down)


def hidden_kernel(cap, pitch, meta_ref, *refs):
    tok_hbm, (gate_hbm, up_hbm, out_ref, tok, rows, gate_w, up_w, tok_sem, gate_sem, up_sem) = refs[:4], refs[4:]
    e = pl.program_id(0)
    n_exp = pl.num_programs(0)
    width = out_ref.shape[2]
    d_model = tok.shape[2]
    top_k = meta_ref.shape[1] // 2
    spans = [slice(start, min(start + SPAN, width)) for start in range(0, width, SPAN)]
    n_buf = gate_w.shape[0]
    now = lax.rem(e, n_buf)
    first = (lax.axis_index("ep") * n_exp) * cap

    def load_tok(s):
        return pltpu.make_async_copy(tok_hbm[s], tok.at[s], tok_sem.at[s])

    def load(i):
        slot = lax.rem(i, n_buf)
        return (
            pltpu.make_async_copy(gate_hbm.at[i], gate_w.at[slot], gate_sem.at[slot]),
            pltpu.make_async_copy(up_hbm.at[i], up_w.at[slot], up_sem.at[slot]),
        )

    def pick_rows(batch, source):
        slot = meta_ref[source, :top_k].astype(jnp.int32) - (first + batch * (BATCH * cap))
        row = lax.broadcasted_iota(jnp.int32, (BATCH * cap, slot.shape[1]), 0)
        hit = row == slot[0:1, :]
        for j in range(1, top_k):
            hit = hit | (row == slot[j : j + 1, :])
        pick = jnp.where(hit, 1.0, 0.0).astype(jnp.bfloat16)
        place = pl.ds(pl.multiple_of(source * pitch, pitch), cap)
        for start in range(0, d_model, 512):
            picked = jnp.dot(pick, tok[source, :, start : start + 512], preferred_element_type=jnp.float32)
            for k in range(BATCH):
                part = picked[k * cap : (k + 1) * cap].astype(jnp.bfloat16)
                rows[lax.rem(batch, 2), k, place, start : start + 512] = part

    @pl.when(e == 0)
    def _():
        for s in range(4):
            load_tok(s).start()
        for i in range(n_buf - 1):
            for copy in load(i):
                copy.start()
        for s in range(4):
            load_tok(s).wait()
        pl.loop(0, 4)(lambda s: pick_rows(0, s))

    @pl.when(e + n_buf - 1 < n_exp)
    def _():
        for copy in load(e + n_buf - 1):
            copy.start()

    @pl.when(e // BATCH < (n_exp - 1) // BATCH)
    def _():
        pick_rows(e // BATCH + 1, lax.rem(e, BATCH))

    for copy in load(e):
        copy.wait()

    mine = [meta_ref[source, :top_k].astype(jnp.int32) - (first + e * cap) for source in range(4)]
    last = jnp.max(jnp.stack([jnp.where(slot < cap, slot, -1) for slot in mine]))
    batch, k = lax.rem(e // BATCH, 2), lax.rem(e, BATCH)

    def swiglu_cols(x, cols):
        gate_pre = jnp.dot(x, gate_w[now, :, cols], preferred_element_type=jnp.float32)
        up_pre = jnp.dot(x, up_w[now, :, cols], preferred_element_type=jnp.float32)
        return jax.nn.silu(gate_pre) * up_pre

    @pl.when(last < FEW_SLOTS)
    def _():
        x = jnp.concatenate([rows[batch, k, s * pitch : s * pitch + FEW_SLOTS] for s in range(4)], axis=0)
        for cols in spans:
            hidden = swiglu_cols(x, cols)
            gap = jnp.zeros((cap - FEW_SLOTS, hidden.shape[1]), jnp.float32)
            pieces = []
            for s in range(4):
                pieces += [hidden[s * FEW_SLOTS : (s + 1) * FEW_SLOTS], gap]
            out_ref[0, :, cols] = jnp.concatenate(pieces, axis=0).astype(jnp.bfloat16)

    @pl.when(last >= FEW_SLOTS)
    def _():
        x = rows[batch, k]
        for cols in spans:
            hidden = swiglu_cols(x, cols)
            pieces = [hidden[s * pitch : s * pitch + cap] for s in range(4)]
            out_ref[0, :, cols] = jnp.concatenate(pieces, axis=0).astype(jnp.bfloat16)


def expert_hidden(metas, sources, w_gate, w_up, cap):
    local_exp, d_model, width = w_gate.shape
    tok_dev = sources[0].shape[0]
    pitch = 16 * ((cap + 15) // 16)
    rows = 4 * cap
    return pl.pallas_call(
        functools.partial(hidden_kernel, cap, pitch),
        grid=(local_exp,),
        in_specs=[pl.BlockSpec(metas.shape, lambda e: (0, 0, 0))] + [ANY] * 6,
        out_specs=pl.BlockSpec((1, rows, width), lambda e: (e, 0, 0)),
        scratch_shapes=[
            pltpu.VMEM((4, tok_dev, d_model), jnp.bfloat16),
            pltpu.VMEM((2, BATCH, 4 * pitch, d_model), jnp.bfloat16),
            pltpu.VMEM((BUFFERS, d_model, width), jnp.bfloat16),
            pltpu.VMEM((BUFFERS, d_model, width), jnp.bfloat16),
            pltpu.SemaphoreType.DMA((4,)),
            pltpu.SemaphoreType.DMA((BUFFERS,)),
            pltpu.SemaphoreType.DMA((BUFFERS,)),
        ],
        out_shape=jax.ShapeDtypeStruct((local_exp, rows, width), jnp.bfloat16),
        compiler_params=params(),
        cost_estimate=cost(local_exp * rows * d_model * width * 4, local_exp * d_model * width * 4),
        name="expert_hidden",
    )(metas, *sources, w_gate, w_up)


def finish_kernel(
    cap, span, n_blocks, combine_hbm, peer_hbm, hidden_hbm, base_ref, weight_ref, shared_ref, out_hbm,
    combine, peer, hidden, rows, kept, given, for_tp, from_core, from_chip, from_tp, out,
    peer_sem, combine_sem, hidden_sem, store_sem, core_send, core_recv, chip_send, chip_recv, tp_send, tp_recv,
):
    step, group = pl.program_id(0), pl.program_id(1)
    n_groups = combine.shape[1]
    n_steps = 2 * n_blocks
    tok_dev, cols = base_ref.shape
    core_peer, chip_peer, _, tp_peer = peers()
    load_peer = pltpu.make_async_copy(peer_hbm, peer, peer_sem)
    old_group = lax.rem(group + n_groups - 1, n_groups)
    old_step = (step * n_groups + group - 1) // n_groups
    slot = lax.rem(step * n_groups + group, 2)
    done = step - 1

    def load_combine(near, g):
        return [
            pltpu.make_async_copy(
                combine_hbm.at[g, pl.ds((half if near else 2 + half) * tok_dev, tok_dev)], combine.at[half, g], combine_sem.at[half, g]
            )
            for half in range(2)
        ]

    def load_hidden(near, g):
        experts = pl.ds(g * GROUP, GROUP)
        source = pl.ds(0 if near else 2 * cap, 2 * cap)
        return pltpu.make_async_copy(hidden_hbm.at[experts, source], hidden.at[experts], hidden_sem.at[g])

    def core_copy(i):
        return pltpu.make_async_remote_copy(
            src_ref=given.at[lax.rem(i, 2)], dst_ref=from_core.at[i],
            send_sem=core_send.at[i], recv_sem=core_recv.at[i], device_id=core_peer, device_id_type=MESH,
        )

    def chip_copy(n):
        return pltpu.make_async_remote_copy(
            src_ref=from_core.at[n], dst_ref=from_chip.at[n],
            send_sem=chip_send.at[n], recv_sem=chip_recv.at[n], device_id=chip_peer, device_id_type=MESH,
        )

    def tp_copy(n):
        return pltpu.make_async_remote_copy(
            src_ref=for_tp.at[n], dst_ref=from_tp.at[n],
            send_sem=tp_send.at[n], recv_sem=tp_recv.at[n], device_id=tp_peer, device_id_type=MESH,
        )

    def store(n):
        here = pl.ds(pl.multiple_of(n * cols, cols), cols)
        return pltpu.make_async_copy(out.at[n], out_hbm.at[:, here], store_sem.at[n])

    def finalize(n):
        chip_copy(n).wait()
        tp_copy(n).wait()
        out[n] = (from_core[n_blocks + n] + from_chip[n] + from_tp[n]).astype(jnp.bfloat16)
        store(n).start()

    def expert_rows():
        results = []
        for k in range(GROUP):
            results.append(jnp.dot(hidden[group * GROUP + k], weight_ref[k], preferred_element_type=jnp.float32))
        gap = jnp.zeros((span - GROUP * cap, cols), jnp.float32)
        for half in range(2):
            part = jnp.concatenate([r[half * cap : (half + 1) * cap] for r in results] + [gap], axis=0)
            rows[slot, half] = part.astype(jnp.bfloat16)

    def add_gated():
        for half, sums in enumerate((kept, given)):
            r = rows[1 - slot, half]
            stacked = jnp.concatenate([r, r, r], axis=0)
            more = jnp.dot(combine[half, old_group], stacked, preferred_element_type=jnp.float32)
            place = lax.rem(old_step, 2)
            sums[place] = jnp.where(old_group == 0, 0.0, sums[place]) + more

    @pl.when((step == 0) & (group == 0))
    def _():
        for g in range(hidden_sem.shape[0]):
            load_hidden(False, g).start()
        load_peer.start()
        for g in range(hidden_sem.shape[0]):
            for copy in load_combine(False, g):
                copy.start()
        greet((core_peer, chip_peer, tp_peer))

    for near in (False, True):
        first = n_blocks if near else 0

        @pl.when(step == first)
        def _():
            load_hidden(near, group).wait()

        @pl.when((old_step == first) & (step + group >= 1))
        def _():
            for copy in load_combine(near, old_group):
                copy.wait()

    @pl.when((step == 0) & (group == 0))
    def _():
        expert_rows()

    @pl.when((step + group >= 1) & (step < n_steps))
    def _():
        add_gated()
        expert_rows()

    @pl.when((step == n_steps) & (group == 0))
    def _():
        add_gated()

    @pl.when(step == n_blocks - 1)
    def _():
        load_hidden(True, group).start()

    @pl.when(old_step == n_blocks - 1)
    def _():
        for copy in load_combine(True, old_group):
            copy.start()

    @pl.when((step >= 1) & (group == 0))
    def _():
        core_copy(done).start()

    @pl.when((step >= 1) & (group == 2))
    def _():
        core_copy(done).wait()
        from_core[done] += kept[lax.rem(done, 2)]

    @pl.when((step >= 1) & (step <= n_blocks) & (group == 2))
    def _():
        chip_copy(done).start()

    @pl.when((step > n_blocks) & (group == 2))
    def _():
        from_core[done] += base_ref[...]

    @pl.when((step == 0) & (group == 1))
    def _():
        load_peer.wait()

    @pl.when((step < n_blocks) & (group == 1))
    def _():
        for_tp[step] = jnp.dot(peer[...], shared_ref[...], preferred_element_type=jnp.float32)
        tp_copy(step).start()

    @pl.when((step > n_blocks) & (step <= n_blocks + 4) & (group == 2))
    def _():
        finalize(done - n_blocks)

    @pl.when((step == n_steps) & (group == 2))
    def _():
        for n in range(4, n_blocks):
            finalize(n)
        for n in range(n_blocks):
            store(n).wait()


def finish(hidden, combine, base, peer_hidden, w_down, shared_down_w):
    local_exp, n_rows, width = hidden.shape
    n_groups = local_exp // GROUP
    cap = n_rows // 4
    depth = combine.shape[2]
    tok_dev, d_model = base.shape
    shared_width = peer_hidden.shape[1]
    cols = d_model // COL_BLOCKS
    sems = pltpu.SemaphoreType.DMA((COL_BLOCKS,))
    two_sems = pltpu.SemaphoreType.DMA((2 * COL_BLOCKS,))
    blocks = (COL_BLOCKS, tok_dev, cols)

    def weight_map(i, g):
        running = i < 2 * COL_BLOCKS
        return jnp.where(running, g, n_groups - 1), 0, jnp.where(running, lax.rem(i, COL_BLOCKS), COL_BLOCKS - 1)

    return pl.pallas_call(
        functools.partial(finish_kernel, cap, depth // 3, COL_BLOCKS),
        grid=(2 * COL_BLOCKS + 1, n_groups),
        out_shape=jax.ShapeDtypeStruct((tok_dev, d_model), jnp.bfloat16),
        in_specs=[
            ANY,
            ANY,
            ANY,
            pl.BlockSpec((tok_dev, cols), lambda i, g: (0, jnp.maximum(i - COL_BLOCKS - 1, 0))),
            pl.BlockSpec((GROUP, width, cols), weight_map),
            pl.BlockSpec((shared_width, cols), lambda i, g: (0, jnp.minimum(i, COL_BLOCKS - 1))),
        ],
        out_specs=ANY,
        scratch_shapes=[
            pltpu.VMEM((2, n_groups, tok_dev, depth), jnp.bfloat16),
            pltpu.VMEM(peer_hidden.shape, jnp.bfloat16),
            pltpu.VMEM((local_exp, 2 * cap, width), jnp.bfloat16),
            pltpu.VMEM((2, 2, depth // 3, cols), jnp.bfloat16),
            pltpu.VMEM((2, tok_dev, cols), jnp.float32),
            pltpu.VMEM((2, tok_dev, cols), jnp.float32),
            pltpu.VMEM(blocks, jnp.float32),
            pltpu.VMEM((2 * COL_BLOCKS, tok_dev, cols), jnp.float32),
            pltpu.VMEM(blocks, jnp.float32),
            pltpu.VMEM(blocks, jnp.float32),
            pltpu.VMEM(blocks, jnp.bfloat16),
            pltpu.SemaphoreType.DMA,
            pltpu.SemaphoreType.DMA((2, n_groups)),
            pltpu.SemaphoreType.DMA((n_groups,)),
            sems, two_sems, two_sems, sems, sems, sems, sems,
        ],
        compiler_params=pltpu.CompilerParams(
            collective_id=0, has_side_effects=True, vmem_limit_bytes=67043328, dimension_semantics=("arbitrary", "arbitrary")
        ),
        cost_estimate=cost(2 * d_model * local_exp * (n_rows * width + 4 * tok_dev * 256), 2 * local_exp * width * d_model),
        name="finish",
    )(combine, peer_hidden, hidden, base, w_down, shared_down_w)


def solution(mesh):
    ep_size = mesh.shape["ep"]
    row_spec = P(("dp", "ep", "tp"), None)
    expert_spec = P("ep", None, None)

    def local_layer(tokens, expert_ids, gates, slots, shared_w1, shared_w3, shared_w2, expert_w1, expert_w3, expert_w2):
        tok_dev, d_model = tokens.shape
        top_k = expert_ids.shape[1]
        local_exp = expert_w1.shape[0]
        cap = capacity_rows(tok_dev, top_k, local_exp * ep_size)
        code = jnp.where(slots >= 0, expert_ids * cap + slots, -1)
        meta = jnp.concatenate([code.astype(jnp.float32).T, gates.T], axis=0)
        _, owner, slot = lane_tables(cap, local_exp)
        metas, tok_core, tok_chip, tok_both, combine, base, peer_hidden = start(meta, owner, slot, tokens, shared_w1, shared_w3, shared_w2, cap, local_exp)
        hidden = expert_hidden(metas, (tokens, tok_core, tok_chip, tok_both), expert_w1, expert_w3, cap)
        return finish(hidden, combine, base, peer_hidden, expert_w2, shared_w2)

    return jax.shard_map(local_layer, mesh=mesh, in_specs=(row_spec, row_spec, row_spec, row_spec, P(None, "tp"), P(None, "tp"), P("tp", None), expert_spec, expert_spec, expert_spec), out_specs=row_spec, check_vma=False)
```

```python
import functools

import jax
import jax.numpy as jnp
from jax import lax
from jax.experimental import pallas as pl
from jax.experimental.pallas import tpu as pltpu
from jax.sharding import PartitionSpec as P
import numpy as np

COL_BLOCKS = 8
GROUP = 5
BATCH = 4
BUFFERS = 3
FEW_SLOTS = 48
SPAN = 512
CHUNK = 128
MESH = pl.DeviceIdType.MESH
GATE_MAX = 3.3895313892515355e38


def capacity_rows(tok_dev, top_k, n_exp):
    return 8 * max(1, (2 * tok_dev * top_k + 8 * n_exp - 1) // (8 * n_exp))


ANY = pl.BlockSpec(memory_space=pl.ANY)


def params():
    return pltpu.CompilerParams(vmem_limit_bytes=62 * 2**20)


def cost(flops, nbytes):
    return pl.CostEstimate(flops=flops, bytes_accessed=nbytes, transcendentals=0)


def peers():
    dp, tp, me = lax.axis_index("dp"), lax.axis_index("tp"), lax.axis_index("ep")
    core = me + 1 - 2 * lax.rem(me, 2)
    chip = lax.rem(me + 2, 4)
    both = lax.rem(core + 2, 4)
    return (dp, tp, core), (dp, tp, chip), (dp, tp, both), (dp, 1 - tp, me)


def greet(devices):
    barrier = pltpu.get_barrier_semaphore()
    for device in devices:
        pl.semaphore_signal(barrier, inc=1, device_id=device, device_id_type=MESH)
    pl.semaphore_wait(barrier, len(devices))


def lane_tables(cap, local_exp):
    span = 128 * ((GROUP * cap + 127) // 128)
    lane = np.arange(local_exp // GROUP * span)
    place = lane % span
    expert = np.where(place < GROUP * cap, lane // span * GROUP + place // cap, -1)
    owner = (np.arange(128)[:, None] == expert[None, :]).astype(np.float32)
    slot = np.where(expert >= 0, place % cap, -1).astype(np.float32)
    return span, jnp.asarray(owner, jnp.bfloat16), jnp.asarray(np.tile(slot, (8, 1)))


def combine_chunk(cap, local_exp, meta, owner_ref, slot_ref, out_ref):
    top_k = meta.shape[0] // 2
    cols = meta.T
    lane = lax.broadcasted_iota(jnp.int32, (CHUNK, 128), 1)
    base = ((lane + lax.axis_index("ep") * local_exp) * cap).astype(jnp.float32)
    slot_of = jnp.full(base.shape, -1024.0, jnp.float32)
    gate = jnp.zeros(base.shape, jnp.float32)
    for j in range(top_k):
        offset = cols[:, j : j + 1] - base
        inside = (offset >= 0.0) & (offset < float(cap)) & (lane < local_exp)
        slot_of = jnp.where(inside, offset, slot_of)
        gate = jnp.where(inside, cols[:, top_k + j : top_k + j + 1], gate)
    high = jnp.minimum(gate, GATE_MAX).astype(jnp.bfloat16).astype(jnp.float32)
    rest = gate - high
    middle = rest.astype(jnp.bfloat16).astype(jnp.float32)
    table = jnp.concatenate([slot_of, high, middle, rest - middle], axis=0).astype(jnp.bfloat16)
    spread = jnp.dot(table, owner_ref[...], preferred_element_type=jnp.float32)
    hit = spread[:CHUNK] == slot_ref[0:1, :]
    n_groups = out_ref.shape[0]
    span = spread.shape[1] // n_groups
    for i in range(3):
        value = jnp.where(hit, spread[(i + 1) * CHUNK : (i + 2) * CHUNK], 0.0).astype(jnp.bfloat16)
        for g in range(n_groups):
            out_ref[g, :, i * span : (i + 1) * span] = value[:, g * span : (g + 1) * span]


def start_kernel(
    cap, local_exp, meta_ref, owner_ref, slot_ref, tok_hbm, w_gate_hbm, w_up_hbm, w_down_hbm,
    metas, tok_core, tok_chip, tok_both, combine_hbm, base_hbm, peer_hbm,
    own, other, own_hidden, peer_hidden, base, w_gate, w_up, w_down,
    load_sem, store_sem, peer_sem, send_sem, recv_sem,
):
    core, chip, both, tp = peers()
    tok_dev, d_model = own.shape
    width = peer_hidden.shape[1]

    def remote(src, dst, device, i):
        return pltpu.make_async_remote_copy(
            src_ref=src, dst_ref=dst, send_sem=send_sem.at[i], recv_sem=recv_sem.at[i], device_id=device, device_id_type=MESH
        )

    greet((core, chip, both, tp))
    meta_copies = [remote(meta_ref, metas.at[i + 1], device, i) for i, device in enumerate((core, chip, both))]
    for copy in meta_copies:
        copy.start()
    to_core = remote(tok_hbm, tok_core, core, 3)
    early = tok_dev // 4 * 3
    parts = [pl.ds(0, early), pl.ds(early, tok_dev - early)]
    to_tp = [remote(tok_hbm.at[part], other.at[part], tp, 4 + i) for i, part in enumerate(parts)]
    to_chip = [remote(tok_hbm.at[part], tok_chip.at[part], chip, 6 + i) for i, part in enumerate(parts)]
    onward = [remote(tok_chip.at[part], tok_both.at[part], core, 8 + i) for i, part in enumerate(parts)]
    for i in range(2):
        to_chip[i].start()
        to_tp[i].start()
    to_core.start()
    pairs = ((tok_hbm, own), (w_gate_hbm, w_gate), (w_up_hbm, w_up), (w_down_hbm, w_down))
    loads = [pltpu.make_async_copy(src, dst, load_sem.at[i]) for i, (src, dst) in enumerate(pairs)]
    for load in loads:
        load.start()
    metas[0] = meta_ref[...]
    for copy in meta_copies:
        copy.wait()

    per_source = tok_dev // CHUNK

    def write_combine(index, out_ref):
        i = index.index[0]
        here = pl.ds(pl.multiple_of(lax.rem(i, per_source) * CHUNK, CHUNK), CHUNK)
        combine_chunk(cap, local_exp, metas[i // per_source, :, here], owner_ref, slot_ref, out_ref)

    n_groups, _, depth = combine_hbm.shape
    pltpu.emit_pipeline(
        write_combine,
        grid=(4 * per_source,),
        out_specs=[pl.BlockSpec((n_groups, CHUNK, depth), lambda i: (0, i, 0))],
        _explicit_indices=True,
    )(combine_hbm)

    def hidden_of(rows, result, here):
        def cols_of(cols):
            gate_pre = jnp.dot(rows[here], w_gate[:, cols], preferred_element_type=jnp.float32)
            up_pre = jnp.dot(rows[here], w_up[:, cols], preferred_element_type=jnp.float32)
            result[here, cols] = (jax.nn.silu(gate_pre) * up_pre).astype(jnp.bfloat16)

        whole = width // SPAN * SPAN

        @pl.loop(0, width // SPAN)
        def _(i):
            cols_of(pl.ds(pl.multiple_of(i * SPAN, SPAN), SPAN))

        if whole < width:
            cols_of(pl.ds(whole, width - whole))

    for load in loads[:3]:
        load.wait()
    hidden_of(own, own_hidden, pl.ds(0, tok_dev))

    def store_peer(i):
        return pltpu.make_async_copy(peer_hidden.at[parts[i]], peer_hbm.at[parts[i]], peer_sem.at[i])

    loads[3].wait()

    @pl.loop(0, d_model // SPAN)
    def _(i):
        cols = pl.ds(pl.multiple_of(i * SPAN, SPAN), SPAN)
        down = jnp.dot(own_hidden[...], w_down[:, cols], preferred_element_type=jnp.float32)
        base[:, cols] = own[:, cols].astype(jnp.float32) + down

    store = pltpu.make_async_copy(base, base_hbm, store_sem)
    store.start()
    for i in range(2):
        to_chip[i].wait()
        onward[i].start()
        to_tp[i].wait()
        hidden_of(other, peer_hidden, parts[i])
        store_peer(i).start()
    for i in range(2):
        store_peer(i).wait()
    store.wait()
    to_core.wait()
    for copy in onward:
        copy.wait()


def start(meta, owner, slot, tokens, w_gate, w_up, w_down, cap, local_exp):
    tok_dev, d_model = tokens.shape
    width = w_gate.shape[1]
    n_groups = local_exp // GROUP
    vmem = pl.BlockSpec(memory_space=pltpu.VMEM)
    tok_shape = jax.ShapeDtypeStruct((tok_dev, d_model), jnp.bfloat16)
    return pl.pallas_call(
        functools.partial(start_kernel, cap, local_exp),
        out_shape=[
            jax.ShapeDtypeStruct((4,) + meta.shape, jnp.float32),
            tok_shape, tok_shape, tok_shape,
            jax.ShapeDtypeStruct((n_groups, 4 * tok_dev, 3 * owner.shape[1] // n_groups), jnp.bfloat16),
            jax.ShapeDtypeStruct((tok_dev, d_model), jnp.float32),
            jax.ShapeDtypeStruct((tok_dev, width), jnp.bfloat16),
        ],
        in_specs=[vmem, vmem, vmem, ANY, ANY, ANY, ANY],
        out_specs=[vmem, ANY, ANY, ANY, ANY, ANY, ANY],
        scratch_shapes=[
            pltpu.VMEM((tok_dev, d_model), jnp.bfloat16),
            pltpu.VMEM((tok_dev, d_model), jnp.bfloat16),
            pltpu.VMEM((tok_dev, width), jnp.bfloat16),
            pltpu.VMEM((tok_dev, width), jnp.bfloat16),
            pltpu.VMEM((tok_dev, d_model), jnp.float32),
            pltpu.VMEM((d_model, width), jnp.bfloat16),
            pltpu.VMEM((d_model, width), jnp.bfloat16),
            pltpu.VMEM((width, d_model), jnp.bfloat16),
            pltpu.SemaphoreType.DMA((4,)),
            pltpu.SemaphoreType.DMA,
            pltpu.SemaphoreType.DMA((2,)),
            pltpu.SemaphoreType.DMA((10,)),
            pltpu.SemaphoreType.DMA((10,)),
        ],
        compiler_params=pltpu.CompilerParams(collective_id=1, has_side_effects=True, vmem_limit_bytes=67043328),
        cost_estimate=cost(10 * tok_dev * d_model * width, 10 * d_model * width),
        name="start",
    )(meta, owner, slot, tokens, w_gate, w_up, w_down)


def hidden_kernel(cap, pitch, meta_ref, *refs):
    tok_hbm, (gate_hbm, up_hbm, out_ref, tok, rows, gate_w, up_w, tok_sem, gate_sem, up_sem) = refs[:4], refs[4:]
    e = pl.program_id(0)
    n_exp = pl.num_programs(0)
    width = out_ref.shape[2]
    d_model = tok.shape[2]
    top_k = meta_ref.shape[1] // 2
    spans = [slice(start, min(start + SPAN, width)) for start in range(0, width, SPAN)]
    n_buf = gate_w.shape[0]
    now = lax.rem(e, n_buf)
    first = (lax.axis_index("ep") * n_exp) * cap

    def load_tok(s):
        return pltpu.make_async_copy(tok_hbm[s], tok.at[s], tok_sem.at[s])

    def load(i):
        slot = lax.rem(i, n_buf)
        return (
            pltpu.make_async_copy(gate_hbm.at[i], gate_w.at[slot], gate_sem.at[slot]),
            pltpu.make_async_copy(up_hbm.at[i], up_w.at[slot], up_sem.at[slot]),
        )

    def pick_rows(batch, source):
        slot = meta_ref[source, :top_k].astype(jnp.int32) - (first + batch * (BATCH * cap))
        row = lax.broadcasted_iota(jnp.int32, (BATCH * cap, slot.shape[1]), 0)
        hit = row == slot[0:1, :]
        for j in range(1, top_k):
            hit = hit | (row == slot[j : j + 1, :])
        pick = jnp.where(hit, 1.0, 0.0).astype(jnp.bfloat16)
        place = pl.ds(pl.multiple_of(source * pitch, pitch), cap)
        for start in range(0, d_model, 512):
            picked = jnp.dot(pick, tok[source, :, start : start + 512], preferred_element_type=jnp.float32)
            for k in range(BATCH):
                part = picked[k * cap : (k + 1) * cap].astype(jnp.bfloat16)
                rows[lax.rem(batch, 2), k, place, start : start + 512] = part

    @pl.when(e == 0)
    def _():
        for s in range(4):
            load_tok(s).start()
        for i in range(n_buf - 1):
            for copy in load(i):
                copy.start()
        for s in range(4):
            load_tok(s).wait()
        pl.loop(0, 4)(lambda s: pick_rows(0, s))

    @pl.when(e + n_buf - 1 < n_exp)
    def _():
        for copy in load(e + n_buf - 1):
            copy.start()

    @pl.when(e // BATCH < (n_exp - 1) // BATCH)
    def _():
        pick_rows(e // BATCH + 1, lax.rem(e, BATCH))

    for copy in load(e):
        copy.wait()

    mine = [meta_ref[source, :top_k].astype(jnp.int32) - (first + e * cap) for source in range(4)]
    last = jnp.max(jnp.stack([jnp.where(slot < cap, slot, -1) for slot in mine]))
    batch, k = lax.rem(e // BATCH, 2), lax.rem(e, BATCH)

    def swiglu_cols(x, cols):
        gate_pre = jnp.dot(x, gate_w[now, :, cols], preferred_element_type=jnp.float32)
        up_pre = jnp.dot(x, up_w[now, :, cols], preferred_element_type=jnp.float32)
        return jax.nn.silu(gate_pre) * up_pre

    @pl.when(last < FEW_SLOTS)
    def _():
        x = jnp.concatenate([rows[batch, k, s * pitch : s * pitch + FEW_SLOTS] for s in range(4)], axis=0)
        for cols in spans:
            hidden = swiglu_cols(x, cols)
            gap = jnp.zeros((cap - FEW_SLOTS, hidden.shape[1]), jnp.float32)
            pieces = []
            for s in range(4):
                pieces += [hidden[s * FEW_SLOTS : (s + 1) * FEW_SLOTS], gap]
            out_ref[0, :, cols] = jnp.concatenate(pieces, axis=0).astype(jnp.bfloat16)

    @pl.when(last >= FEW_SLOTS)
    def _():
        x = rows[batch, k]
        for cols in spans:
            hidden = swiglu_cols(x, cols)
            pieces = [hidden[s * pitch : s * pitch + cap] for s in range(4)]
            out_ref[0, :, cols] = jnp.concatenate(pieces, axis=0).astype(jnp.bfloat16)


def expert_hidden(metas, sources, w_gate, w_up, cap):
    local_exp, d_model, width = w_gate.shape
    tok_dev = sources[0].shape[0]
    pitch = 16 * ((cap + 15) // 16)
    rows = 4 * cap
    return pl.pallas_call(
        functools.partial(hidden_kernel, cap, pitch),
        grid=(local_exp,),
        in_specs=[pl.BlockSpec(metas.shape, lambda e: (0, 0, 0))] + [ANY] * 6,
        out_specs=pl.BlockSpec((1, rows, width), lambda e: (e, 0, 0)),
        scratch_shapes=[
            pltpu.VMEM((4, tok_dev, d_model), jnp.bfloat16),
            pltpu.VMEM((2, BATCH, 4 * pitch, d_model), jnp.bfloat16),
            pltpu.VMEM((BUFFERS, d_model, width), jnp.bfloat16),
            pltpu.VMEM((BUFFERS, d_model, width), jnp.bfloat16),
            pltpu.SemaphoreType.DMA((4,)),
            pltpu.SemaphoreType.DMA((BUFFERS,)),
            pltpu.SemaphoreType.DMA((BUFFERS,)),
        ],
        out_shape=jax.ShapeDtypeStruct((local_exp, rows, width), jnp.bfloat16),
        compiler_params=params(),
        cost_estimate=cost(local_exp * rows * d_model * width * 4, local_exp * d_model * width * 4),
        name="expert_hidden",
    )(metas, *sources, w_gate, w_up)


def finish_kernel(
    cap, span, n_blocks, combine_hbm, peer_hbm, hidden_hbm, weight_hbm, base_hbm, shared_hbm, out_hbm,
    base, shared, combine, peer, hidden, weight, rows, kept, given, for_tp, from_core, from_chip, from_tp, out,
    base_sem, shared_sem, peer_sem, combine_sem, hidden_sem, weight_sem, store_sem, core_send, core_recv, chip_send, chip_recv, tp_send, tp_recv,
):
    step = pl.program_id(0)
    n_groups = combine.shape[1]
    n_steps = 2 * n_blocks
    tok_dev, cols = base.shape[1:]
    core_peer, chip_peer, _, tp_peer = peers()
    load_peer = pltpu.make_async_copy(peer_hbm, peer, peer_sem)
    done = step - 1

    def load_combine(near, g):
        return [
            pltpu.make_async_copy(
                combine_hbm.at[g, pl.ds((half if near else 2 + half) * tok_dev, tok_dev)], combine.at[half, g], combine_sem.at[half, g]
            )
            for half in range(2)
        ]

    def load_hidden(near, g):
        experts = pl.ds(g * GROUP, GROUP)
        source = pl.ds(0 if near else 2 * cap, 2 * cap)
        return pltpu.make_async_copy(hidden_hbm.at[experts, source], hidden.at[experts], hidden_sem.at[g])

    def load_weight(i, g):
        here = pl.ds(pl.multiple_of(lax.rem(i, n_blocks) * cols, cols), cols)
        return pltpu.make_async_copy(weight_hbm.at[pl.ds(g * GROUP, GROUP), :, here], weight.at[g], weight_sem.at[g])

    def cols_of(n):
        return pl.ds(pl.multiple_of(n * cols, cols), cols)

    def load_base(n):
        slot = lax.rem(n, 2)
        return pltpu.make_async_copy(base_hbm.at[:, cols_of(n)], base.at[slot], base_sem.at[slot])

    def load_shared(n):
        slot = lax.rem(n, 2)
        return pltpu.make_async_copy(shared_hbm.at[:, cols_of(n)], shared.at[slot], shared_sem.at[slot])

    def core_copy(i):
        return pltpu.make_async_remote_copy(
            src_ref=given.at[lax.rem(i, 2)], dst_ref=from_core.at[i],
            send_sem=core_send.at[i], recv_sem=core_recv.at[i], device_id=core_peer, device_id_type=MESH,
        )

    def chip_copy(n):
        return pltpu.make_async_remote_copy(
            src_ref=from_core.at[n], dst_ref=from_chip.at[n],
            send_sem=chip_send.at[n], recv_sem=chip_recv.at[n], device_id=chip_peer, device_id_type=MESH,
        )

    def tp_copy(n):
        return pltpu.make_async_remote_copy(
            src_ref=for_tp.at[n], dst_ref=from_tp.at[n],
            send_sem=tp_send.at[n], recv_sem=tp_recv.at[n], device_id=tp_peer, device_id_type=MESH,
        )

    def store(n):
        here = pl.ds(pl.multiple_of(n * cols, cols), cols)
        return pltpu.make_async_copy(out.at[n], out_hbm.at[:, here], store_sem.at[n])

    def finalize(n):
        chip_copy(n).wait()
        tp_copy(n).wait()
        out[n] = (from_core[n_blocks + n] + from_chip[n] + from_tp[n]).astype(jnp.bfloat16)
        store(n).start()

    def expert_rows(g):
        results = []
        for k in range(GROUP):
            results.append(jnp.dot(hidden[g * GROUP + k], weight[g, k], preferred_element_type=jnp.float32))
        gap = jnp.zeros((span - GROUP * cap, cols), jnp.float32)
        for half in range(2):
            part = jnp.concatenate([r[half * cap : (half + 1) * cap] for r in results] + [gap], axis=0)
            rows[g, half] = part.astype(jnp.bfloat16)

    def add_gated(i, g):
        place = lax.rem(i, 2)
        for half, sums in enumerate((kept, given)):
            r = rows[g, half]
            more = jnp.dot(combine[half, g], jnp.concatenate([r, r, r], axis=0), preferred_element_type=jnp.float32)
            sums[place] = more if g == 0 else sums[place] + more

    def share_peer():
        load_shared(step).wait()
        for_tp[step] = jnp.dot(peer[...], shared[lax.rem(step, 2)], preferred_element_type=jnp.float32)
        tp_copy(step).start()

    @pl.when(step == 0)
    def _():
        load_hidden(False, 0).start()
        load_weight(step, 0).start()
        load_hidden(False, 1).start()
        load_weight(step, 1).start()
        for copy in load_combine(False, 0):
            copy.start()
        greet((core_peer, chip_peer, tp_peer))

    def ready(i, g):
        for near in (False, True):

            @pl.when(i == (n_blocks if near else 0))
            def _():
                for copy in load_combine(near, g):
                    copy.wait()

    def hidden_ready(g):
        for near in (False, True):

            @pl.when(step == (n_blocks if near else 0))
            def _():
                load_hidden(near, g).wait()

    def refill(g):
        @pl.when(step < n_steps - 1)
        def _():
            load_weight(step + 1, g).start()

        @pl.when(step == n_blocks - 1)
        def _():
            load_hidden(True, g).start()

    def refill_combine(i, g):
        @pl.when(i == n_blocks - 1)
        def _():
            for copy in load_combine(True, g):
                copy.start()

    last = n_groups - 1
    hidden_ready(0)
    ready(done, last)

    @pl.when(step == 0)
    def _():
        load_weight(step, 0).wait()
        for g in range(2, n_groups):
            load_hidden(False, g).start()
            load_weight(step, g).start()
        for g in range(1, n_groups):
            for copy in load_combine(False, g):
                copy.start()
        load_peer.start()
        load_shared(step).start()
        expert_rows(0)

    @pl.when((step > 0) & (step < n_steps))
    def _():
        add_gated(done, last)
        core_copy(done).start()
        load_weight(step, 0).wait()
        expert_rows(0)

    @pl.when(step == n_steps)
    def _():
        add_gated(done, last)
        core_copy(done).start()

    refill(0)
    refill_combine(done, last)

    @pl.when((step >= 1) & (step <= n_blocks))
    def _():
        core_copy(done).wait()
        from_core[done] += kept[lax.rem(done, 2)]
        chip_copy(done).start()

    @pl.when(step > n_blocks)
    def _():
        core_copy(done).wait()
        load_base(done - n_blocks).wait()
        from_core[done] += kept[lax.rem(done, 2)] + base[lax.rem(done, 2)]

    for g in range(1, n_groups):
        hidden_ready(g)
        ready(step, g - 1)

        @pl.when(step < n_steps)
        def _():
            load_weight(step, g).wait()
            add_gated(step, g - 1)
            expert_rows(g)

        refill(g)
        refill_combine(step, g - 1)

        if g == 1:

            @pl.when(step == 0)
            def _():
                load_peer.wait()

            @pl.when(step < n_blocks - 1)
            def _():
                load_shared(step + 1).start()

            @pl.when(step < n_blocks)
            def _():
                share_peer()

            @pl.when((step >= n_blocks) & (step < n_steps))
            def _():
                load_base(step - n_blocks).start()

    @pl.when((step > n_blocks) & (step <= n_blocks + 4))
    def _():
        finalize(done - n_blocks)

    @pl.when(step == n_steps)
    def _():
        for n in range(4, n_blocks):
            finalize(n)
        for n in range(n_blocks):
            store(n).wait()


def finish(hidden, combine, base, peer_hidden, w_down, shared_down_w):
    local_exp, n_rows, width = hidden.shape
    n_groups = local_exp // GROUP
    cap = n_rows // 4
    depth = combine.shape[2]
    tok_dev, d_model = base.shape
    shared_width = peer_hidden.shape[1]
    cols = d_model // COL_BLOCKS
    sems = pltpu.SemaphoreType.DMA((COL_BLOCKS,))
    two_sems = pltpu.SemaphoreType.DMA((2 * COL_BLOCKS,))
    group_sems = pltpu.SemaphoreType.DMA((n_groups,))
    blocks = (COL_BLOCKS, tok_dev, cols)
    return pl.pallas_call(
        functools.partial(finish_kernel, cap, depth // 3, COL_BLOCKS),
        grid=(2 * COL_BLOCKS + 1,),
        out_shape=jax.ShapeDtypeStruct((tok_dev, d_model), jnp.bfloat16),
        in_specs=[
            ANY
        ]
        * 6,
        out_specs=ANY,
        scratch_shapes=[
            pltpu.VMEM((2, tok_dev, cols), jnp.float32),
            pltpu.VMEM((2, shared_width, cols), jnp.bfloat16),
            pltpu.VMEM((2, n_groups, tok_dev, depth), jnp.bfloat16),
            pltpu.VMEM(peer_hidden.shape, jnp.bfloat16),
            pltpu.VMEM((local_exp, 2 * cap, width), jnp.bfloat16),
            pltpu.VMEM((n_groups, GROUP, width, cols), jnp.bfloat16),
            pltpu.VMEM((n_groups, 2, depth // 3, cols), jnp.bfloat16),
            pltpu.VMEM((2, tok_dev, cols), jnp.float32),
            pltpu.VMEM((2, tok_dev, cols), jnp.float32),
            pltpu.VMEM(blocks, jnp.float32),
            pltpu.VMEM((2 * COL_BLOCKS, tok_dev, cols), jnp.float32),
            pltpu.VMEM(blocks, jnp.float32),
            pltpu.VMEM(blocks, jnp.float32),
            pltpu.VMEM(blocks, jnp.bfloat16),
            pltpu.SemaphoreType.DMA((2,)),
            pltpu.SemaphoreType.DMA((2,)),
            pltpu.SemaphoreType.DMA,
            pltpu.SemaphoreType.DMA((2, n_groups)),
            group_sems,
            group_sems,
            sems, two_sems, two_sems, sems, sems, sems, sems,
        ],
        compiler_params=pltpu.CompilerParams(
            collective_id=0, has_side_effects=True, vmem_limit_bytes=67043328, dimension_semantics=("arbitrary",)
        ),
        cost_estimate=cost(2 * d_model * local_exp * (n_rows * width + 4 * tok_dev * 256), 2 * local_exp * width * d_model),
        name="finish",
    )(combine, peer_hidden, hidden, w_down, base, shared_down_w)


def solution(mesh):
    ep_size = mesh.shape["ep"]
    row_spec = P(("dp", "ep", "tp"), None)
    expert_spec = P("ep", None, None)

    def local_layer(tokens, expert_ids, gates, slots, shared_w1, shared_w3, shared_w2, expert_w1, expert_w3, expert_w2):
        tok_dev, d_model = tokens.shape
        top_k = expert_ids.shape[1]
        local_exp = expert_w1.shape[0]
        cap = capacity_rows(tok_dev, top_k, local_exp * ep_size)
        code = jnp.where(slots >= 0, expert_ids * cap + slots, -1)
        meta = jnp.concatenate([code.astype(jnp.float32).T, gates.T], axis=0)
        _, owner, slot = lane_tables(cap, local_exp)
        metas, tok_core, tok_chip, tok_both, combine, base, peer_hidden = start(meta, owner, slot, tokens, shared_w1, shared_w3, shared_w2, cap, local_exp)
        hidden = expert_hidden(metas, (tokens, tok_core, tok_chip, tok_both), expert_w1, expert_w3, cap)
        return finish(hidden, combine, base, peer_hidden, expert_w2, shared_w2)

    return jax.shard_map(local_layer, mesh=mesh, in_specs=(row_spec, row_spec, row_spec, row_spec, P(None, "tp"), P(None, "tp"), P("tp", None), expert_spec, expert_spec, expert_spec), out_specs=row_spec, check_vma=False)
```

```python
import functools

import jax
import jax.numpy as jnp
from jax import lax
from jax.experimental import pallas as pl
from jax.experimental.pallas import tpu as pltpu
from jax.sharding import PartitionSpec as P
import numpy as np

COL_BLOCKS = 8
GROUP = 5
BATCH = 4
BUFFERS = 3
FEW_SLOTS = 48
SPAN = 512
CHUNK = 128
MESH = pl.DeviceIdType.MESH
GATE_MAX = 3.3895313892515355e38


def capacity_rows(tok_dev, top_k, n_exp):
    return 8 * max(1, (2 * tok_dev * top_k + 8 * n_exp - 1) // (8 * n_exp))


ANY = pl.BlockSpec(memory_space=pl.ANY)


def params():
    return pltpu.CompilerParams(vmem_limit_bytes=62 * 2**20)


def cost(flops, nbytes):
    return pl.CostEstimate(flops=flops, bytes_accessed=nbytes, transcendentals=0)


def peers():
    dp, tp, me = lax.axis_index("dp"), lax.axis_index("tp"), lax.axis_index("ep")
    core = me + 1 - 2 * lax.rem(me, 2)
    chip = lax.rem(me + 2, 4)
    both = lax.rem(core + 2, 4)
    return (dp, tp, core), (dp, tp, chip), (dp, tp, both), (dp, 1 - tp, me)


def greet(devices):
    barrier = pltpu.get_barrier_semaphore()
    for device in devices:
        pl.semaphore_signal(barrier, inc=1, device_id=device, device_id_type=MESH)
    pl.semaphore_wait(barrier, len(devices))


def lane_tables(cap, local_exp):
    span = 128 * ((GROUP * cap + 127) // 128)
    lane = np.arange(local_exp // GROUP * span)
    place = lane % span
    expert = np.where(place < GROUP * cap, lane // span * GROUP + place // cap, -1)
    owner = (np.arange(128)[:, None] == expert[None, :]).astype(np.float32)
    slot = np.where(expert >= 0, place % cap, -1).astype(np.float32)
    return span, jnp.asarray(owner, jnp.bfloat16), jnp.asarray(np.tile(slot, (8, 1)))


def combine_chunk(cap, local_exp, meta, owner_ref, slot_ref, out_ref):
    top_k = meta.shape[0] // 2
    cols = meta.T
    lane = lax.broadcasted_iota(jnp.int32, (CHUNK, 128), 1)
    base = ((lane + lax.axis_index("ep") * local_exp) * cap).astype(jnp.float32)
    slot_of = jnp.full(base.shape, -1024.0, jnp.float32)
    gate = jnp.zeros(base.shape, jnp.float32)
    for j in range(top_k):
        offset = cols[:, j : j + 1] - base
        inside = (offset >= 0.0) & (offset < float(cap)) & (lane < local_exp)
        slot_of = jnp.where(inside, offset, slot_of)
        gate = jnp.where(inside, cols[:, top_k + j : top_k + j + 1], gate)
    high = jnp.minimum(gate, GATE_MAX).astype(jnp.bfloat16).astype(jnp.float32)
    rest = gate - high
    middle = rest.astype(jnp.bfloat16).astype(jnp.float32)
    table = jnp.concatenate([slot_of, high, middle, rest - middle], axis=0).astype(jnp.bfloat16)
    spread = jnp.dot(table, owner_ref[...], preferred_element_type=jnp.float32)
    hit = spread[:CHUNK] == slot_ref[0:1, :]
    n_groups = out_ref.shape[0]
    span = spread.shape[1] // n_groups
    for i in range(3):
        value = jnp.where(hit, spread[(i + 1) * CHUNK : (i + 2) * CHUNK], 0.0).astype(jnp.bfloat16)
        for g in range(n_groups):
            out_ref[g, :, i * span : (i + 1) * span] = value[:, g * span : (g + 1) * span]


def start_kernel(
    cap, local_exp, meta_ref, owner_ref, slot_ref, tok_hbm, w_gate_hbm, w_up_hbm, w_down_hbm,
    metas, tok_core, tok_chip, tok_both, combine_hbm, base_hbm, peer_hbm,
    own, other, own_hidden, peer_hidden, base, w_gate, w_up, w_down,
    load_sem, store_sem, peer_sem, send_sem, recv_sem,
):
    core, chip, both, tp = peers()
    tok_dev, d_model = own.shape
    width = peer_hidden.shape[1]

    def remote(src, dst, device, i):
        return pltpu.make_async_remote_copy(
            src_ref=src, dst_ref=dst, send_sem=send_sem.at[i], recv_sem=recv_sem.at[i], device_id=device, device_id_type=MESH
        )

    greet((core, chip, both, tp))
    meta_copies = [remote(meta_ref, metas.at[i + 1], device, i) for i, device in enumerate((core, chip, both))]
    for copy in meta_copies:
        copy.start()
    to_core = remote(tok_hbm, tok_core, core, 3)
    early = tok_dev // 4 * 3
    parts = [pl.ds(0, early), pl.ds(early, tok_dev - early)]
    to_tp = [remote(tok_hbm.at[part], other.at[part], tp, 4 + i) for i, part in enumerate(parts)]
    to_chip = [remote(tok_hbm.at[part], tok_chip.at[part], chip, 6 + i) for i, part in enumerate(parts)]
    onward = [remote(tok_chip.at[part], tok_both.at[part], core, 8 + i) for i, part in enumerate(parts)]
    for i in range(2):
        to_chip[i].start()
        to_tp[i].start()
    to_core.start()
    pairs = ((tok_hbm, own), (w_gate_hbm, w_gate), (w_up_hbm, w_up), (w_down_hbm, w_down))
    loads = [pltpu.make_async_copy(src, dst, load_sem.at[i]) for i, (src, dst) in enumerate(pairs)]
    for load in loads:
        load.start()
    metas[0] = meta_ref[...]
    for copy in meta_copies:
        copy.wait()

    per_source = tok_dev // CHUNK

    def write_combine(index, out_ref):
        i = index.index[0]
        here = pl.ds(pl.multiple_of(lax.rem(i, per_source) * CHUNK, CHUNK), CHUNK)
        combine_chunk(cap, local_exp, metas[i // per_source, :, here], owner_ref, slot_ref, out_ref)

    n_groups, _, depth = combine_hbm.shape
    pltpu.emit_pipeline(
        write_combine,
        grid=(4 * per_source,),
        out_specs=[pl.BlockSpec((n_groups, CHUNK, depth), lambda i: (0, i, 0))],
        _explicit_indices=True,
    )(combine_hbm)

    def hidden_of(rows, result, here):
        def cols_of(cols):
            gate_pre = jnp.dot(rows[here], w_gate[:, cols], preferred_element_type=jnp.float32)
            up_pre = jnp.dot(rows[here], w_up[:, cols], preferred_element_type=jnp.float32)
            result[here, cols] = (jax.nn.silu(gate_pre) * up_pre).astype(jnp.bfloat16)

        whole = width // SPAN * SPAN

        @pl.loop(0, width // SPAN)
        def _(i):
            cols_of(pl.ds(pl.multiple_of(i * SPAN, SPAN), SPAN))

        if whole < width:
            cols_of(pl.ds(whole, width - whole))

    for load in loads[:3]:
        load.wait()
    hidden_of(own, own_hidden, pl.ds(0, tok_dev))

    def store_peer(i):
        return pltpu.make_async_copy(peer_hidden.at[parts[i]], peer_hbm.at[parts[i]], peer_sem.at[i])

    loads[3].wait()

    @pl.loop(0, d_model // SPAN)
    def _(i):
        cols = pl.ds(pl.multiple_of(i * SPAN, SPAN), SPAN)
        down = jnp.dot(own_hidden[...], w_down[:, cols], preferred_element_type=jnp.float32)
        base[:, cols] = own[:, cols].astype(jnp.float32) + down

    store = pltpu.make_async_copy(base, base_hbm, store_sem)
    store.start()
    for i in range(2):
        to_chip[i].wait()
        onward[i].start()
        to_tp[i].wait()
        hidden_of(other, peer_hidden, parts[i])
        store_peer(i).start()
    for i in range(2):
        store_peer(i).wait()
    store.wait()
    to_core.wait()
    for copy in onward:
        copy.wait()


def start(meta, owner, slot, tokens, w_gate, w_up, w_down, cap, local_exp):
    tok_dev, d_model = tokens.shape
    width = w_gate.shape[1]
    n_groups = local_exp // GROUP
    vmem = pl.BlockSpec(memory_space=pltpu.VMEM)
    tok_shape = jax.ShapeDtypeStruct((tok_dev, d_model), jnp.bfloat16)
    return pl.pallas_call(
        functools.partial(start_kernel, cap, local_exp),
        out_shape=[
            jax.ShapeDtypeStruct((4,) + meta.shape, jnp.float32),
            tok_shape, tok_shape, tok_shape,
            jax.ShapeDtypeStruct((n_groups, 4 * tok_dev, 3 * owner.shape[1] // n_groups), jnp.bfloat16),
            jax.ShapeDtypeStruct((tok_dev, d_model), jnp.float32),
            jax.ShapeDtypeStruct((tok_dev, width), jnp.bfloat16),
        ],
        in_specs=[vmem, vmem, vmem, ANY, ANY, ANY, ANY],
        out_specs=[vmem, ANY, ANY, ANY, ANY, ANY, ANY],
        scratch_shapes=[
            pltpu.VMEM((tok_dev, d_model), jnp.bfloat16),
            pltpu.VMEM((tok_dev, d_model), jnp.bfloat16),
            pltpu.VMEM((tok_dev, width), jnp.bfloat16),
            pltpu.VMEM((tok_dev, width), jnp.bfloat16),
            pltpu.VMEM((tok_dev, d_model), jnp.float32),
            pltpu.VMEM((d_model, width), jnp.bfloat16),
            pltpu.VMEM((d_model, width), jnp.bfloat16),
            pltpu.VMEM((width, d_model), jnp.bfloat16),
            pltpu.SemaphoreType.DMA((4,)),
            pltpu.SemaphoreType.DMA,
            pltpu.SemaphoreType.DMA((2,)),
            pltpu.SemaphoreType.DMA((10,)),
            pltpu.SemaphoreType.DMA((10,)),
        ],
        compiler_params=pltpu.CompilerParams(collective_id=1, has_side_effects=True, vmem_limit_bytes=67043328),
        cost_estimate=cost(10 * tok_dev * d_model * width, 10 * d_model * width),
        name="start",
    )(meta, owner, slot, tokens, w_gate, w_up, w_down)


def hidden_kernel(cap, pitch, meta_ref, *refs):
    tok_hbm, (gate_hbm, up_hbm, out_ref, tok, rows, gate_w, up_w, tok_sem, gate_sem, up_sem) = refs[:4], refs[4:]
    e = pl.program_id(0)
    n_exp = pl.num_programs(0)
    width = out_ref.shape[2]
    d_model = tok.shape[2]
    top_k = meta_ref.shape[1] // 2
    spans = [slice(start, min(start + SPAN, width)) for start in range(0, width, SPAN)]
    n_buf = gate_w.shape[0]
    now = lax.rem(e, n_buf)
    first = (lax.axis_index("ep") * n_exp) * cap

    def load_tok(s):
        return pltpu.make_async_copy(tok_hbm[s], tok.at[s], tok_sem.at[s])

    def load(i):
        slot = lax.rem(i, n_buf)
        return (
            pltpu.make_async_copy(gate_hbm.at[i], gate_w.at[slot], gate_sem.at[slot]),
            pltpu.make_async_copy(up_hbm.at[i], up_w.at[slot], up_sem.at[slot]),
        )

    def pick_rows(batch, source):
        slot = meta_ref[source, :top_k].astype(jnp.int32) - (first + batch * (BATCH * cap))
        row = lax.broadcasted_iota(jnp.int32, (BATCH * cap, slot.shape[1]), 0)
        hit = row == slot[0:1, :]
        for j in range(1, top_k):
            hit = hit | (row == slot[j : j + 1, :])
        pick = jnp.where(hit, 1.0, 0.0).astype(jnp.bfloat16)
        place = pl.ds(pl.multiple_of(source * pitch, pitch), cap)
        for start in range(0, d_model, 512):
            picked = jnp.dot(pick, tok[source, :, start : start + 512], preferred_element_type=jnp.float32)
            for k in range(BATCH):
                part = picked[k * cap : (k + 1) * cap].astype(jnp.bfloat16)
                rows[lax.rem(batch, 2), k, place, start : start + 512] = part

    @pl.when(e == 0)
    def _():
        for s in range(4):
            load_tok(s).start()
        for i in range(n_buf - 1):
            for copy in load(i):
                copy.start()
        for s in range(4):
            load_tok(s).wait()
        pl.loop(0, 4)(lambda s: pick_rows(0, s))

    @pl.when(e + n_buf - 1 < n_exp)
    def _():
        for copy in load(e + n_buf - 1):
            copy.start()

    @pl.when(e // BATCH < (n_exp - 1) // BATCH)
    def _():
        pick_rows(e // BATCH + 1, lax.rem(e, BATCH))

    for copy in load(e):
        copy.wait()

    mine = [meta_ref[source, :top_k].astype(jnp.int32) - (first + e * cap) for source in range(4)]
    last = jnp.max(jnp.stack([jnp.where(slot < cap, slot, -1) for slot in mine]))
    batch, k = lax.rem(e // BATCH, 2), lax.rem(e, BATCH)

    def swiglu_cols(x, cols):
        gate_pre = jnp.dot(x, gate_w[now, :, cols], preferred_element_type=jnp.float32)
        up_pre = jnp.dot(x, up_w[now, :, cols], preferred_element_type=jnp.float32)
        return jax.nn.silu(gate_pre) * up_pre

    @pl.when(last < FEW_SLOTS)
    def _():
        x = jnp.concatenate([rows[batch, k, s * pitch : s * pitch + FEW_SLOTS] for s in range(4)], axis=0)
        for cols in spans:
            hidden = swiglu_cols(x, cols)
            gap = jnp.zeros((cap - FEW_SLOTS, hidden.shape[1]), jnp.float32)
            pieces = []
            for s in range(4):
                pieces += [hidden[s * FEW_SLOTS : (s + 1) * FEW_SLOTS], gap]
            out_ref[0, :, cols] = jnp.concatenate(pieces, axis=0).astype(jnp.bfloat16)

    @pl.when(last >= FEW_SLOTS)
    def _():
        x = rows[batch, k]
        for cols in spans:
            hidden = swiglu_cols(x, cols)
            pieces = [hidden[s * pitch : s * pitch + cap] for s in range(4)]
            out_ref[0, :, cols] = jnp.concatenate(pieces, axis=0).astype(jnp.bfloat16)


def expert_hidden(metas, sources, w_gate, w_up, cap):
    local_exp, d_model, width = w_gate.shape
    tok_dev = sources[0].shape[0]
    pitch = 16 * ((cap + 15) // 16)
    rows = 4 * cap
    return pl.pallas_call(
        functools.partial(hidden_kernel, cap, pitch),
        grid=(local_exp,),
        in_specs=[pl.BlockSpec(metas.shape, lambda e: (0, 0, 0))] + [ANY] * 6,
        out_specs=pl.BlockSpec((1, rows, width), lambda e: (e, 0, 0)),
        scratch_shapes=[
            pltpu.VMEM((4, tok_dev, d_model), jnp.bfloat16),
            pltpu.VMEM((2, BATCH, 4 * pitch, d_model), jnp.bfloat16),
            pltpu.VMEM((BUFFERS, d_model, width), jnp.bfloat16),
            pltpu.VMEM((BUFFERS, d_model, width), jnp.bfloat16),
            pltpu.SemaphoreType.DMA((4,)),
            pltpu.SemaphoreType.DMA((BUFFERS,)),
            pltpu.SemaphoreType.DMA((BUFFERS,)),
        ],
        out_shape=jax.ShapeDtypeStruct((local_exp, rows, width), jnp.bfloat16),
        compiler_params=params(),
        cost_estimate=cost(local_exp * rows * d_model * width * 4, local_exp * d_model * width * 4),
        name="expert_hidden",
    )(metas, *sources, w_gate, w_up)


def finish_kernel(
    cap, span, n_blocks, combine_hbm, peer_hbm, hidden_hbm, weight_hbm, base_hbm, shared_hbm, out_hbm,
    base, shared, combine, peer, hidden, weight, rows, kept, given, for_tp, from_core, from_chip, from_tp, out,
    base_sem, shared_sem, peer_sem, combine_sem, hidden_sem, weight_sem, store_sem, core_send, core_recv, chip_send, chip_recv, tp_send, tp_recv,
):
    step = pl.program_id(0)
    n_groups = combine.shape[1]
    n_steps = 2 * n_blocks
    tok_dev, cols = base.shape[1:]
    core_peer, chip_peer, _, tp_peer = peers()
    load_peer = pltpu.make_async_copy(peer_hbm, peer, peer_sem)
    done = step - 1

    def load_combine(near, g):
        return [
            pltpu.make_async_copy(
                combine_hbm.at[g, pl.ds((half if near else 2 + half) * tok_dev, tok_dev)], combine.at[half, g], combine_sem.at[half, g]
            )
            for half in range(2)
        ]

    def load_hidden(near, g):
        experts = pl.ds(g * GROUP, GROUP)
        source = pl.ds(0 if near else 2 * cap, 2 * cap)
        return pltpu.make_async_copy(hidden_hbm.at[experts, source], hidden.at[experts], hidden_sem.at[g])

    def load_weight(i, g):
        here = pl.ds(pl.multiple_of(lax.rem(i, n_blocks) * cols, cols), cols)
        return pltpu.make_async_copy(weight_hbm.at[pl.ds(g * GROUP, GROUP), :, here], weight.at[g], weight_sem.at[g])

    def cols_of(n):
        return pl.ds(pl.multiple_of(n * cols, cols), cols)

    def load_base(n):
        slot = lax.rem(n, 2)
        return pltpu.make_async_copy(base_hbm.at[:, cols_of(n)], base.at[slot], base_sem.at[slot])

    def load_shared(n):
        slot = lax.rem(n, 2)
        return pltpu.make_async_copy(shared_hbm.at[:, cols_of(n)], shared.at[slot], shared_sem.at[slot])

    def core_copy(i):
        return pltpu.make_async_remote_copy(
            src_ref=given.at[lax.rem(i, 2)], dst_ref=from_core.at[i],
            send_sem=core_send.at[i], recv_sem=core_recv.at[i], device_id=core_peer, device_id_type=MESH,
        )

    def chip_copy(n):
        return pltpu.make_async_remote_copy(
            src_ref=from_core.at[n], dst_ref=from_chip.at[n],
            send_sem=chip_send.at[n], recv_sem=chip_recv.at[n], device_id=chip_peer, device_id_type=MESH,
        )

    def tp_copy(n):
        return pltpu.make_async_remote_copy(
            src_ref=for_tp.at[n], dst_ref=from_tp.at[n],
            send_sem=tp_send.at[n], recv_sem=tp_recv.at[n], device_id=tp_peer, device_id_type=MESH,
        )

    def store(n):
        here = pl.ds(pl.multiple_of(n * cols, cols), cols)
        return pltpu.make_async_copy(out.at[n], out_hbm.at[:, here], store_sem.at[n])

    def finalize(n):
        chip_copy(n).wait()
        tp_copy(n).wait()
        out[n] = (from_core[n_blocks + n] + from_chip[n] + from_tp[n]).astype(jnp.bfloat16)
        store(n).start()

    def expert_rows(g):
        results = []
        for k in range(GROUP):
            results.append(jnp.dot(hidden[g * GROUP + k], weight[g, k], preferred_element_type=jnp.float32))
        gap = jnp.zeros((span - GROUP * cap, cols), jnp.float32)
        for half in range(2):
            part = jnp.concatenate([r[half * cap : (half + 1) * cap] for r in results] + [gap], axis=0)
            rows[g, half] = part.astype(jnp.bfloat16)

    def add_gated(i, g):
        place = lax.rem(i, 2)
        for half, sums in enumerate((kept, given)):
            r = rows[g, half]
            more = jnp.dot(combine[half, g], jnp.concatenate([r, r, r], axis=0), preferred_element_type=jnp.float32)
            sums[place] = more if g == 0 else sums[place] + more

    def share_peer():
        load_shared(step).wait()
        for_tp[step] = jnp.dot(peer[...], shared[lax.rem(step, 2)], preferred_element_type=jnp.float32)
        tp_copy(step).start()

    @pl.when(step == 0)
    def _():
        load_hidden(False, 0).start()
        load_weight(step, 0).start()
        load_peer.start()
        load_shared(step).start()
        load_hidden(False, 1).start()
        load_weight(step, 1).start()
        for copy in load_combine(False, 0):
            copy.start()
        greet((core_peer, chip_peer, tp_peer))

    def ready(i, g):
        for near in (False, True):

            @pl.when(i == (n_blocks if near else 0))
            def _():
                for copy in load_combine(near, g):
                    copy.wait()

    def hidden_ready(g):
        for near in (False, True):

            @pl.when(step == (n_blocks if near else 0))
            def _():
                load_hidden(near, g).wait()

    def refill(g):
        @pl.when(step < n_steps - 1)
        def _():
            load_weight(step + 1, g).start()

        @pl.when(step == n_blocks - 1)
        def _():
            load_hidden(True, g).start()

    def refill_combine(i, g):
        @pl.when(i == n_blocks - 1)
        def _():
            for copy in load_combine(True, g):
                copy.start()

    last = n_groups - 1
    hidden_ready(0)
    ready(done, last)

    @pl.when(step == 0)
    def _():
        load_weight(step, 0).wait()
        for g in range(2, n_groups):
            load_hidden(False, g).start()
            load_weight(step, g).start()
        for g in range(1, n_groups):
            for copy in load_combine(False, g):
                copy.start()
        expert_rows(0)
        load_peer.wait()
        share_peer()

    @pl.when((step > 0) & (step < n_steps))
    def _():
        add_gated(done, last)
        core_copy(done).start()
        load_weight(step, 0).wait()
        expert_rows(0)

    @pl.when(step == n_steps)
    def _():
        add_gated(done, last)
        core_copy(done).start()

    refill(0)
    refill_combine(done, last)

    def forward():
        core_copy(done).wait()
        from_core[done] += kept[lax.rem(done, 2)]
        chip_copy(done).start()

    def keep():
        core_copy(done).wait()
        load_base(done - n_blocks).wait()
        from_core[done] += kept[lax.rem(done, 2)] + base[lax.rem(done, 2)]

    pl.when(step == 1)(forward)

    for g in range(1, n_groups):
        hidden_ready(g)
        ready(step, g - 1)

        @pl.when(step < n_steps)
        def _():
            load_weight(step, g).wait()
            add_gated(step, g - 1)
            expert_rows(g)

        refill(g)
        refill_combine(step, g - 1)

        if g == 1:

            @pl.when(step < n_blocks - 1)
            def _():
                load_shared(step + 1).start()

            @pl.when((step > 0) & (step < n_blocks))
            def _():
                share_peer()

            @pl.when((step >= n_blocks) & (step < n_steps))
            def _():
                load_base(step - n_blocks).start()

    pl.when((step > 1) & (step <= n_blocks))(forward)
    pl.when(step > n_blocks)(keep)

    @pl.when((step > n_blocks) & (step <= n_blocks + 4))
    def _():
        finalize(done - n_blocks)

    @pl.when(step == n_steps)
    def _():
        for n in range(4, n_blocks):
            finalize(n)
        for n in range(n_blocks):
            store(n).wait()


def finish(hidden, combine, base, peer_hidden, w_down, shared_down_w):
    local_exp, n_rows, width = hidden.shape
    n_groups = local_exp // GROUP
    cap = n_rows // 4
    depth = combine.shape[2]
    tok_dev, d_model = base.shape
    shared_width = peer_hidden.shape[1]
    cols = d_model // COL_BLOCKS
    sems = pltpu.SemaphoreType.DMA((COL_BLOCKS,))
    two_sems = pltpu.SemaphoreType.DMA((2 * COL_BLOCKS,))
    group_sems = pltpu.SemaphoreType.DMA((n_groups,))
    blocks = (COL_BLOCKS, tok_dev, cols)
    return pl.pallas_call(
        functools.partial(finish_kernel, cap, depth // 3, COL_BLOCKS),
        grid=(2 * COL_BLOCKS + 1,),
        out_shape=jax.ShapeDtypeStruct((tok_dev, d_model), jnp.bfloat16),
        in_specs=[
            ANY
        ]
        * 6,
        out_specs=ANY,
        scratch_shapes=[
            pltpu.VMEM((2, tok_dev, cols), jnp.float32),
            pltpu.VMEM((2, shared_width, cols), jnp.bfloat16),
            pltpu.VMEM((2, n_groups, tok_dev, depth), jnp.bfloat16),
            pltpu.VMEM(peer_hidden.shape, jnp.bfloat16),
            pltpu.VMEM((local_exp, 2 * cap, width), jnp.bfloat16),
            pltpu.VMEM((n_groups, GROUP, width, cols), jnp.bfloat16),
            pltpu.VMEM((n_groups, 2, depth // 3, cols), jnp.bfloat16),
            pltpu.VMEM((2, tok_dev, cols), jnp.float32),
            pltpu.VMEM((2, tok_dev, cols), jnp.float32),
            pltpu.VMEM(blocks, jnp.float32),
            pltpu.VMEM((2 * COL_BLOCKS, tok_dev, cols), jnp.float32),
            pltpu.VMEM(blocks, jnp.float32),
            pltpu.VMEM(blocks, jnp.float32),
            pltpu.VMEM(blocks, jnp.bfloat16),
            pltpu.SemaphoreType.DMA((2,)),
            pltpu.SemaphoreType.DMA((2,)),
            pltpu.SemaphoreType.DMA,
            pltpu.SemaphoreType.DMA((2, n_groups)),
            group_sems,
            group_sems,
            sems, two_sems, two_sems, sems, sems, sems, sems,
        ],
        compiler_params=pltpu.CompilerParams(
            collective_id=0, has_side_effects=True, vmem_limit_bytes=67043328, dimension_semantics=("arbitrary",)
        ),
        cost_estimate=cost(2 * d_model * local_exp * (n_rows * width + 4 * tok_dev * 256), 2 * local_exp * width * d_model),
        name="finish",
    )(combine, peer_hidden, hidden, w_down, base, shared_down_w)


def solution(mesh):
    ep_size = mesh.shape["ep"]
    row_spec = P(("dp", "ep", "tp"), None)
    expert_spec = P("ep", None, None)

    def local_layer(tokens, expert_ids, gates, slots, shared_w1, shared_w3, shared_w2, expert_w1, expert_w3, expert_w2):
        tok_dev, d_model = tokens.shape
        top_k = expert_ids.shape[1]
        local_exp = expert_w1.shape[0]
        cap = capacity_rows(tok_dev, top_k, local_exp * ep_size)
        code = jnp.where(slots >= 0, expert_ids * cap + slots, -1)
        meta = jnp.concatenate([code.astype(jnp.float32).T, gates.T], axis=0)
        _, owner, slot = lane_tables(cap, local_exp)
        metas, tok_core, tok_chip, tok_both, combine, base, peer_hidden = start(meta, owner, slot, tokens, shared_w1, shared_w3, shared_w2, cap, local_exp)
        hidden = expert_hidden(metas, (tokens, tok_core, tok_chip, tok_both), expert_w1, expert_w3, cap)
        return finish(hidden, combine, base, peer_hidden, expert_w2, shared_w2)

    return jax.shard_map(local_layer, mesh=mesh, in_specs=(row_spec, row_spec, row_spec, row_spec, P(None, "tp"), P(None, "tp"), P("tp", None), expert_spec, expert_spec, expert_spec), out_specs=row_spec, check_vma=False)
```

```python
import functools

import jax
import jax.numpy as jnp
from jax import lax
from jax.experimental import pallas as pl
from jax.experimental.pallas import tpu as pltpu
from jax.sharding import PartitionSpec as P
import numpy as np

COL_BLOCKS = 8
GROUP = 5
BATCH = 4
BUFFERS = 3
FEW_SLOTS = 48
SPAN = 512
CHUNK = 128
MESH = pl.DeviceIdType.MESH
GATE_MAX = 3.3895313892515355e38


def capacity_rows(tok_dev, top_k, n_exp):
    return 8 * max(1, (2 * tok_dev * top_k + 8 * n_exp - 1) // (8 * n_exp))


ANY = pl.BlockSpec(memory_space=pl.ANY)


def params():
    return pltpu.CompilerParams(vmem_limit_bytes=62 * 2**20)


def cost(flops, nbytes):
    return pl.CostEstimate(flops=flops, bytes_accessed=nbytes, transcendentals=0)


def peers():
    dp, tp, me = lax.axis_index("dp"), lax.axis_index("tp"), lax.axis_index("ep")
    core = me + 1 - 2 * lax.rem(me, 2)
    chip = lax.rem(me + 2, 4)
    both = lax.rem(core + 2, 4)
    return (dp, tp, core), (dp, tp, chip), (dp, tp, both), (dp, 1 - tp, me)


def greet(devices):
    barrier = pltpu.get_barrier_semaphore()
    for device in devices:
        pl.semaphore_signal(barrier, inc=1, device_id=device, device_id_type=MESH)
    pl.semaphore_wait(barrier, len(devices))


def lane_tables(cap, local_exp):
    span = 128 * ((GROUP * cap + 127) // 128)
    lane = np.arange(local_exp // GROUP * span)
    place = lane % span
    expert = np.where(place < GROUP * cap, lane // span * GROUP + place // cap, -1)
    owner = (np.arange(128)[:, None] == expert[None, :]).astype(np.float32)
    slot = np.where(expert >= 0, place % cap, -1).astype(np.float32)
    return span, jnp.asarray(owner, jnp.bfloat16), jnp.asarray(np.tile(slot, (8, 1)))


def combine_chunk(cap, local_exp, meta, owner_ref, slot_ref, out_ref):
    top_k = meta.shape[0] // 2
    cols = meta.T
    lane = lax.broadcasted_iota(jnp.int32, (CHUNK, 128), 1)
    base = ((lane + lax.axis_index("ep") * local_exp) * cap).astype(jnp.float32)
    slot_of = jnp.full(base.shape, -1024.0, jnp.float32)
    gate = jnp.zeros(base.shape, jnp.float32)
    for j in range(top_k):
        offset = cols[:, j : j + 1] - base
        inside = (offset >= 0.0) & (offset < float(cap)) & (lane < local_exp)
        slot_of = jnp.where(inside, offset, slot_of)
        gate = jnp.where(inside, cols[:, top_k + j : top_k + j + 1], gate)
    high = jnp.minimum(gate, GATE_MAX).astype(jnp.bfloat16).astype(jnp.float32)
    rest = gate - high
    middle = rest.astype(jnp.bfloat16).astype(jnp.float32)
    table = jnp.concatenate([slot_of, high, middle, rest - middle], axis=0).astype(jnp.bfloat16)
    spread = jnp.dot(table, owner_ref[...], preferred_element_type=jnp.float32)
    hit = spread[:CHUNK] == slot_ref[0:1, :]
    n_groups = out_ref.shape[0]
    span = spread.shape[1] // n_groups
    for i in range(3):
        value = jnp.where(hit, spread[(i + 1) * CHUNK : (i + 2) * CHUNK], 0.0).astype(jnp.bfloat16)
        for g in range(n_groups):
            out_ref[g, :, i * span : (i + 1) * span] = value[:, g * span : (g + 1) * span]


def start_kernel(
    cap, local_exp, id_ref, gate_ref, slots_ref, owner_ref, slot_ref, tok_hbm, w_gate_hbm, w_up_hbm, w_down_hbm,
    metas, tok_core, tok_chip, tok_both, combine_hbm, base_hbm, peer_hbm,
    own, other, own_hidden, peer_hidden, base, w_gate, w_up, w_down,
    load_sem, store_sem, peer_sem, send_sem, recv_sem,
):
    core, chip, both, tp = peers()
    tok_dev, d_model = own.shape
    width = peer_hidden.shape[1]

    def remote(src, dst, device, i):
        return pltpu.make_async_remote_copy(
            src_ref=src, dst_ref=dst, send_sem=send_sem.at[i], recv_sem=recv_sem.at[i], device_id=device, device_id_type=MESH
        )

    ids, slots = id_ref[...], slots_ref[...]
    code = jnp.where(slots >= 0, ids * cap + slots, -1).astype(jnp.float32)
    top_k = code.shape[0]
    metas[0, :top_k] = code
    metas[0, top_k:] = gate_ref[...]
    greet((core, chip, both, tp))
    meta_copies = [remote(metas.at[0], metas.at[i + 1], device, i) for i, device in enumerate((core, chip, both))]
    for copy in meta_copies:
        copy.start()
    to_core = remote(tok_hbm, tok_core, core, 3)
    early = tok_dev // 4 * 3
    parts = [pl.ds(0, early), pl.ds(early, tok_dev - early)]
    to_tp = [remote(tok_hbm.at[part], other.at[part], tp, 4 + i) for i, part in enumerate(parts)]
    to_chip = [remote(tok_hbm.at[part], tok_chip.at[part], chip, 6 + i) for i, part in enumerate(parts)]
    onward = [remote(tok_chip.at[part], tok_both.at[part], core, 8 + i) for i, part in enumerate(parts)]
    for i in range(2):
        to_chip[i].start()
        to_tp[i].start()
    to_core.start()
    pairs = ((tok_hbm, own), (w_gate_hbm, w_gate), (w_up_hbm, w_up), (w_down_hbm, w_down))
    loads = [pltpu.make_async_copy(src, dst, load_sem.at[i]) for i, (src, dst) in enumerate(pairs)]
    for load in loads:
        load.start()
    for copy in meta_copies:
        copy.wait()

    per_source = tok_dev // CHUNK

    def write_combine(index, out_ref):
        i = index.index[0]
        here = pl.ds(pl.multiple_of(lax.rem(i, per_source) * CHUNK, CHUNK), CHUNK)
        combine_chunk(cap, local_exp, metas[i // per_source, :, here], owner_ref, slot_ref, out_ref)

    n_groups, _, depth = combine_hbm.shape
    pltpu.emit_pipeline(
        write_combine,
        grid=(4 * per_source,),
        out_specs=[pl.BlockSpec((n_groups, CHUNK, depth), lambda i: (0, i, 0))],
        _explicit_indices=True,
    )(combine_hbm)

    def hidden_of(rows, result, here):
        def cols_of(cols):
            gate_pre = jnp.dot(rows[here], w_gate[:, cols], preferred_element_type=jnp.float32)
            up_pre = jnp.dot(rows[here], w_up[:, cols], preferred_element_type=jnp.float32)
            result[here, cols] = (jax.nn.silu(gate_pre) * up_pre).astype(jnp.bfloat16)

        whole = width // SPAN * SPAN

        @pl.loop(0, width // SPAN)
        def _(i):
            cols_of(pl.ds(pl.multiple_of(i * SPAN, SPAN), SPAN))

        if whole < width:
            cols_of(pl.ds(whole, width - whole))

    for load in loads[:3]:
        load.wait()
    hidden_of(own, own_hidden, pl.ds(0, tok_dev))

    def store_peer(i):
        return pltpu.make_async_copy(peer_hidden.at[parts[i]], peer_hbm.at[parts[i]], peer_sem.at[i])

    loads[3].wait()

    @pl.loop(0, d_model // SPAN)
    def _(i):
        cols = pl.ds(pl.multiple_of(i * SPAN, SPAN), SPAN)
        down = jnp.dot(own_hidden[...], w_down[:, cols], preferred_element_type=jnp.float32)
        base[:, cols] = own[:, cols].astype(jnp.float32) + down

    store = pltpu.make_async_copy(base, base_hbm, store_sem)
    store.start()
    for i in range(2):
        to_chip[i].wait()
        onward[i].start()
        to_tp[i].wait()
        hidden_of(other, peer_hidden, parts[i])
        store_peer(i).start()
    for i in range(2):
        store_peer(i).wait()
    store.wait()
    to_core.wait()
    for copy in onward:
        copy.wait()


def start(ids, gates, slots, owner, slot, tokens, w_gate, w_up, w_down, cap, local_exp):
    tok_dev, d_model = tokens.shape
    width = w_gate.shape[1]
    n_groups = local_exp // GROUP
    vmem = pl.BlockSpec(memory_space=pltpu.VMEM)
    tok_shape = jax.ShapeDtypeStruct((tok_dev, d_model), jnp.bfloat16)
    return pl.pallas_call(
        functools.partial(start_kernel, cap, local_exp),
        out_shape=[
            jax.ShapeDtypeStruct((4, 2 * ids.shape[0], tok_dev), jnp.float32),
            tok_shape, tok_shape, tok_shape,
            jax.ShapeDtypeStruct((n_groups, 4 * tok_dev, 3 * owner.shape[1] // n_groups), jnp.bfloat16),
            jax.ShapeDtypeStruct((tok_dev, d_model), jnp.float32),
            jax.ShapeDtypeStruct((tok_dev, width), jnp.bfloat16),
        ],
        in_specs=[vmem] * 5 + [ANY] * 4,
        out_specs=[vmem, ANY, ANY, ANY, ANY, ANY, ANY],
        scratch_shapes=[
            pltpu.VMEM((tok_dev, d_model), jnp.bfloat16),
            pltpu.VMEM((tok_dev, d_model), jnp.bfloat16),
            pltpu.VMEM((tok_dev, width), jnp.bfloat16),
            pltpu.VMEM((tok_dev, width), jnp.bfloat16),
            pltpu.VMEM((tok_dev, d_model), jnp.float32),
            pltpu.VMEM((d_model, width), jnp.bfloat16),
            pltpu.VMEM((d_model, width), jnp.bfloat16),
            pltpu.VMEM((width, d_model), jnp.bfloat16),
            pltpu.SemaphoreType.DMA((4,)),
            pltpu.SemaphoreType.DMA,
            pltpu.SemaphoreType.DMA((2,)),
            pltpu.SemaphoreType.DMA((10,)),
            pltpu.SemaphoreType.DMA((10,)),
        ],
        compiler_params=pltpu.CompilerParams(collective_id=1, has_side_effects=True, vmem_limit_bytes=67043328),
        cost_estimate=cost(10 * tok_dev * d_model * width, 10 * d_model * width),
        name="start",
    )(ids, gates, slots, owner, slot, tokens, w_gate, w_up, w_down)


def hidden_kernel(cap, pitch, meta_ref, *refs):
    tok_hbm, (gate_hbm, up_hbm, out_ref, tok, rows, gate_w, up_w, tok_sem, gate_sem, up_sem) = refs[:4], refs[4:]
    e = pl.program_id(0)
    n_exp = pl.num_programs(0)
    width = out_ref.shape[2]
    d_model = tok.shape[2]
    top_k = meta_ref.shape[1] // 2
    spans = [slice(start, min(start + SPAN, width)) for start in range(0, width, SPAN)]
    n_buf = gate_w.shape[0]
    now = lax.rem(e, n_buf)
    first = (lax.axis_index("ep") * n_exp) * cap

    def load_tok(s):
        return pltpu.make_async_copy(tok_hbm[s], tok.at[s], tok_sem.at[s])

    def load(i):
        slot = lax.rem(i, n_buf)
        return (
            pltpu.make_async_copy(gate_hbm.at[i], gate_w.at[slot], gate_sem.at[slot]),
            pltpu.make_async_copy(up_hbm.at[i], up_w.at[slot], up_sem.at[slot]),
        )

    def pick_rows(batch, source):
        slot = meta_ref[source, :top_k].astype(jnp.int32) - (first + batch * (BATCH * cap))
        row = lax.broadcasted_iota(jnp.int32, (BATCH * cap, slot.shape[1]), 0)
        hit = row == slot[0:1, :]
        for j in range(1, top_k):
            hit = hit | (row == slot[j : j + 1, :])
        pick = jnp.where(hit, 1.0, 0.0).astype(jnp.bfloat16)
        place = pl.ds(pl.multiple_of(source * pitch, pitch), cap)
        for start in range(0, d_model, 512):
            picked = jnp.dot(pick, tok[source, :, start : start + 512], preferred_element_type=jnp.float32)
            for k in range(BATCH):
                part = picked[k * cap : (k + 1) * cap].astype(jnp.bfloat16)
                rows[lax.rem(batch, 2), k, place, start : start + 512] = part

    @pl.when(e == 0)
    def _():
        for s in range(4):
            load_tok(s).start()
        for i in range(n_buf - 1):
            for copy in load(i):
                copy.start()
        for s in range(4):
            load_tok(s).wait()
        pl.loop(0, 4)(lambda s: pick_rows(0, s))

    @pl.when(e + n_buf - 1 < n_exp)
    def _():
        for copy in load(e + n_buf - 1):
            copy.start()

    @pl.when(e // BATCH < (n_exp - 1) // BATCH)
    def _():
        pick_rows(e // BATCH + 1, lax.rem(e, BATCH))

    for copy in load(e):
        copy.wait()

    mine = [meta_ref[source, :top_k].astype(jnp.int32) - (first + e * cap) for source in range(4)]
    last = jnp.max(jnp.stack([jnp.where(slot < cap, slot, -1) for slot in mine]))
    batch, k = lax.rem(e // BATCH, 2), lax.rem(e, BATCH)

    def swiglu_cols(x, cols):
        gate_pre = jnp.dot(x, gate_w[now, :, cols], preferred_element_type=jnp.float32)
        up_pre = jnp.dot(x, up_w[now, :, cols], preferred_element_type=jnp.float32)
        return jax.nn.silu(gate_pre) * up_pre

    @pl.when(last < FEW_SLOTS)
    def _():
        x = jnp.concatenate([rows[batch, k, s * pitch : s * pitch + FEW_SLOTS] for s in range(4)], axis=0)
        for cols in spans:
            hidden = swiglu_cols(x, cols)
            gap = jnp.zeros((cap - FEW_SLOTS, hidden.shape[1]), jnp.float32)
            pieces = []
            for s in range(4):
                pieces += [hidden[s * FEW_SLOTS : (s + 1) * FEW_SLOTS], gap]
            out_ref[0, :, cols] = jnp.concatenate(pieces, axis=0).astype(jnp.bfloat16)

    @pl.when(last >= FEW_SLOTS)
    def _():
        x = rows[batch, k]
        for cols in spans:
            hidden = swiglu_cols(x, cols)
            pieces = [hidden[s * pitch : s * pitch + cap] for s in range(4)]
            out_ref[0, :, cols] = jnp.concatenate(pieces, axis=0).astype(jnp.bfloat16)


def expert_hidden(metas, sources, w_gate, w_up, cap):
    local_exp, d_model, width = w_gate.shape
    tok_dev = sources[0].shape[0]
    pitch = 16 * ((cap + 15) // 16)
    rows = 4 * cap
    return pl.pallas_call(
        functools.partial(hidden_kernel, cap, pitch),
        grid=(local_exp,),
        in_specs=[pl.BlockSpec(metas.shape, lambda e: (0, 0, 0))] + [ANY] * 6,
        out_specs=pl.BlockSpec((1, rows, width), lambda e: (e, 0, 0)),
        scratch_shapes=[
            pltpu.VMEM((4, tok_dev, d_model), jnp.bfloat16),
            pltpu.VMEM((2, BATCH, 4 * pitch, d_model), jnp.bfloat16),
            pltpu.VMEM((BUFFERS, d_model, width), jnp.bfloat16),
            pltpu.VMEM((BUFFERS, d_model, width), jnp.bfloat16),
            pltpu.SemaphoreType.DMA((4,)),
            pltpu.SemaphoreType.DMA((BUFFERS,)),
            pltpu.SemaphoreType.DMA((BUFFERS,)),
        ],
        out_shape=jax.ShapeDtypeStruct((local_exp, rows, width), jnp.bfloat16),
        compiler_params=params(),
        cost_estimate=cost(local_exp * rows * d_model * width * 4, local_exp * d_model * width * 4),
        name="expert_hidden",
    )(metas, *sources, w_gate, w_up)


def finish_kernel(
    cap, span, n_blocks, combine_hbm, peer_hbm, hidden_hbm, weight_hbm, base_hbm, shared_hbm, out_hbm,
    base, shared, combine, peer, hidden, weight, rows, kept, given, for_tp, from_core, from_chip, from_tp, out,
    base_sem, shared_sem, peer_sem, combine_sem, hidden_sem, weight_sem, store_sem, core_send, core_recv, chip_send, chip_recv, tp_send, tp_recv,
):
    step = pl.program_id(0)
    n_groups = combine.shape[1]
    n_steps = 2 * n_blocks
    tok_dev, cols = base.shape[1:]
    core_peer, chip_peer, _, tp_peer = peers()
    load_peer = pltpu.make_async_copy(peer_hbm, peer, peer_sem)
    done = step - 1

    def load_combine(near, g):
        return [
            pltpu.make_async_copy(
                combine_hbm.at[g, pl.ds((half if near else 2 + half) * tok_dev, tok_dev)], combine.at[half, g], combine_sem.at[half, g]
            )
            for half in range(2)
        ]

    def load_hidden(near, g):
        experts = pl.ds(g * GROUP, GROUP)
        source = pl.ds(0 if near else 2 * cap, 2 * cap)
        return pltpu.make_async_copy(hidden_hbm.at[experts, source], hidden.at[experts], hidden_sem.at[g])

    def load_weight(i, g):
        here = pl.ds(pl.multiple_of(lax.rem(i, n_blocks) * cols, cols), cols)
        return pltpu.make_async_copy(weight_hbm.at[pl.ds(g * GROUP, GROUP), :, here], weight.at[g], weight_sem.at[g])

    def cols_of(n):
        return pl.ds(pl.multiple_of(n * cols, cols), cols)

    def load_base(n):
        slot = lax.rem(n, 2)
        return pltpu.make_async_copy(base_hbm.at[:, cols_of(n)], base.at[slot], base_sem.at[slot])

    def load_shared(n):
        slot = lax.rem(n, 2)
        return pltpu.make_async_copy(shared_hbm.at[:, cols_of(n)], shared.at[slot], shared_sem.at[slot])

    def core_copy(i):
        return pltpu.make_async_remote_copy(
            src_ref=given.at[lax.rem(i, 2)], dst_ref=from_core.at[i],
            send_sem=core_send.at[i], recv_sem=core_recv.at[i], device_id=core_peer, device_id_type=MESH,
        )

    def chip_copy(n):
        return pltpu.make_async_remote_copy(
            src_ref=from_core.at[n], dst_ref=from_chip.at[n],
            send_sem=chip_send.at[n], recv_sem=chip_recv.at[n], device_id=chip_peer, device_id_type=MESH,
        )

    def tp_copy(n):
        return pltpu.make_async_remote_copy(
            src_ref=for_tp.at[n], dst_ref=from_tp.at[n],
            send_sem=tp_send.at[n], recv_sem=tp_recv.at[n], device_id=tp_peer, device_id_type=MESH,
        )

    def store(n):
        here = pl.ds(pl.multiple_of(n * cols, cols), cols)
        return pltpu.make_async_copy(out.at[n], out_hbm.at[:, here], store_sem.at[n])

    def finalize(n):
        chip_copy(n).wait()
        tp_copy(n).wait()
        out[n] = (from_core[n_blocks + n] + from_chip[n] + from_tp[n]).astype(jnp.bfloat16)
        store(n).start()

    def expert_rows(g):
        results = []
        for k in range(GROUP):
            results.append(jnp.dot(hidden[g * GROUP + k], weight[g, k], preferred_element_type=jnp.float32))
        gap = jnp.zeros((span - GROUP * cap, cols), jnp.float32)
        for half in range(2):
            part = jnp.concatenate([r[half * cap : (half + 1) * cap] for r in results] + [gap], axis=0)
            rows[g, half] = part.astype(jnp.bfloat16)

    def add_gated(i, g):
        place = lax.rem(i, 2)
        for half, sums in enumerate((kept, given)):
            r = rows[g, half]
            more = jnp.dot(combine[half, g], jnp.concatenate([r, r, r], axis=0), preferred_element_type=jnp.float32)
            sums[place] = more if g == 0 else sums[place] + more

    def share_peer():
        load_shared(step).wait()
        for_tp[step] = jnp.dot(peer[...], shared[lax.rem(step, 2)], preferred_element_type=jnp.float32)
        tp_copy(step).start()

    @pl.when(step == 0)
    def _():
        load_hidden(False, 0).start()
        load_weight(step, 0).start()
        load_peer.start()
        load_shared(step).start()
        load_hidden(False, 1).start()
        load_weight(step, 1).start()
        for copy in load_combine(False, 0):
            copy.start()
        greet((core_peer, chip_peer, tp_peer))

    def ready(i, g):
        for near in (False, True):

            @pl.when(i == (n_blocks if near else 0))
            def _():
                for copy in load_combine(near, g):
                    copy.wait()

    def hidden_ready(g):
        for near in (False, True):

            @pl.when(step == (n_blocks if near else 0))
            def _():
                load_hidden(near, g).wait()

    def refill(g):
        @pl.when(step < n_steps - 1)
        def _():
            load_weight(step + 1, g).start()

        @pl.when(step == n_blocks - 1)
        def _():
            load_hidden(True, g).start()

    def refill_combine(i, g):
        @pl.when(i == n_blocks - 1)
        def _():
            for copy in load_combine(True, g):
                copy.start()

    last = n_groups - 1
    hidden_ready(0)
    ready(done, last)

    @pl.when(step == 0)
    def _():
        load_weight(step, 0).wait()
        for g in range(2, n_groups):
            load_hidden(False, g).start()
            load_weight(step, g).start()
        for g in range(1, n_groups):
            for copy in load_combine(False, g):
                copy.start()
        expert_rows(0)
        load_peer.wait()
        share_peer()

    @pl.when((step > 0) & (step < n_steps))
    def _():
        add_gated(done, last)
        core_copy(done).start()
        load_weight(step, 0).wait()
        expert_rows(0)

    @pl.when(step == n_steps)
    def _():
        add_gated(done, last)
        core_copy(done).start()

    refill(0)
    refill_combine(done, last)

    def forward():
        core_copy(done).wait()
        from_core[done] += kept[lax.rem(done, 2)]
        chip_copy(done).start()

    def keep():
        core_copy(done).wait()
        load_base(done - n_blocks).wait()
        from_core[done] += kept[lax.rem(done, 2)] + base[lax.rem(done, 2)]

    pl.when(step == 1)(forward)

    for g in range(1, n_groups):
        hidden_ready(g)
        ready(step, g - 1)

        @pl.when(step < n_steps)
        def _():
            load_weight(step, g).wait()
            add_gated(step, g - 1)
            expert_rows(g)

        refill(g)
        refill_combine(step, g - 1)

        if g == 1:

            @pl.when(step < n_blocks - 1)
            def _():
                load_shared(step + 1).start()

            @pl.when((step > 0) & (step < n_blocks))
            def _():
                share_peer()

            @pl.when((step >= n_blocks) & (step < n_steps))
            def _():
                load_base(step - n_blocks).start()

    pl.when((step > 1) & (step <= n_blocks))(forward)
    pl.when(step > n_blocks)(keep)

    @pl.when((step > n_blocks) & (step <= n_blocks + 4))
    def _():
        finalize(done - n_blocks)

    @pl.when(step == n_steps)
    def _():
        for n in range(4, n_blocks):
            finalize(n)
        for n in range(n_blocks):
            store(n).wait()


def finish(hidden, combine, base, peer_hidden, w_down, shared_down_w):
    local_exp, n_rows, width = hidden.shape
    n_groups = local_exp // GROUP
    cap = n_rows // 4
    depth = combine.shape[2]
    tok_dev, d_model = base.shape
    shared_width = peer_hidden.shape[1]
    cols = d_model // COL_BLOCKS
    sems = pltpu.SemaphoreType.DMA((COL_BLOCKS,))
    two_sems = pltpu.SemaphoreType.DMA((2 * COL_BLOCKS,))
    group_sems = pltpu.SemaphoreType.DMA((n_groups,))
    blocks = (COL_BLOCKS, tok_dev, cols)
    return pl.pallas_call(
        functools.partial(finish_kernel, cap, depth // 3, COL_BLOCKS),
        grid=(2 * COL_BLOCKS + 1,),
        out_shape=jax.ShapeDtypeStruct((tok_dev, d_model), jnp.bfloat16),
        in_specs=[
            ANY
        ]
        * 6,
        out_specs=ANY,
        scratch_shapes=[
            pltpu.VMEM((2, tok_dev, cols), jnp.float32),
            pltpu.VMEM((2, shared_width, cols), jnp.bfloat16),
            pltpu.VMEM((2, n_groups, tok_dev, depth), jnp.bfloat16),
            pltpu.VMEM(peer_hidden.shape, jnp.bfloat16),
            pltpu.VMEM((local_exp, 2 * cap, width), jnp.bfloat16),
            pltpu.VMEM((n_groups, GROUP, width, cols), jnp.bfloat16),
            pltpu.VMEM((n_groups, 2, depth // 3, cols), jnp.bfloat16),
            pltpu.VMEM((2, tok_dev, cols), jnp.float32),
            pltpu.VMEM((2, tok_dev, cols), jnp.float32),
            pltpu.VMEM(blocks, jnp.float32),
            pltpu.VMEM((2 * COL_BLOCKS, tok_dev, cols), jnp.float32),
            pltpu.VMEM(blocks, jnp.float32),
            pltpu.VMEM(blocks, jnp.float32),
            pltpu.VMEM(blocks, jnp.bfloat16),
            pltpu.SemaphoreType.DMA((2,)),
            pltpu.SemaphoreType.DMA((2,)),
            pltpu.SemaphoreType.DMA,
            pltpu.SemaphoreType.DMA((2, n_groups)),
            group_sems,
            group_sems,
            sems, two_sems, two_sems, sems, sems, sems, sems,
        ],
        compiler_params=pltpu.CompilerParams(
            collective_id=0, has_side_effects=True, vmem_limit_bytes=67043328, dimension_semantics=("arbitrary",)
        ),
        cost_estimate=cost(2 * d_model * local_exp * (n_rows * width + 4 * tok_dev * 256), 2 * local_exp * width * d_model),
        name="finish",
    )(combine, peer_hidden, hidden, w_down, base, shared_down_w)


def solution(mesh):
    ep_size = mesh.shape["ep"]
    row_spec = P(("dp", "ep", "tp"), None)
    expert_spec = P("ep", None, None)

    def local_layer(tokens, expert_ids, gates, slots, shared_w1, shared_w3, shared_w2, expert_w1, expert_w3, expert_w2):
        tok_dev, d_model = tokens.shape
        top_k = expert_ids.shape[1]
        local_exp = expert_w1.shape[0]
        cap = capacity_rows(tok_dev, top_k, local_exp * ep_size)
        _, owner, slot = lane_tables(cap, local_exp)
        metas, tok_core, tok_chip, tok_both, combine, base, peer_hidden = start(expert_ids.T, gates.T, slots.T, owner, slot, tokens, shared_w1, shared_w3, shared_w2, cap, local_exp)
        hidden = expert_hidden(metas, (tokens, tok_core, tok_chip, tok_both), expert_w1, expert_w3, cap)
        return finish(hidden, combine, base, peer_hidden, expert_w2, shared_w2)

    return jax.shard_map(local_layer, mesh=mesh, in_specs=(row_spec, row_spec, row_spec, row_spec, P(None, "tp"), P(None, "tp"), P("tp", None), expert_spec, expert_spec, expert_spec), out_specs=row_spec, check_vma=False)
```
